128 devices in a mesh: row: 8 (over z, core), col: 16 (over x, y).
Axes of the slice: x: 4, y: 4, z: 4, core: 2. Of those that a mesh axis runs over, the one named last changes fastest.
Arguments:
- grad_terms: bfloat16 [16, 2, 4096, 10240], P('col', None, 'row'), may hold values from -25 to 25, as said below
- row_moment: float32 [2, 4096], P(None, 'row'), may hold values from 0.01 to 3
- col_moment: float32 [2, 10240], P(None, 'col'), may hold values from 0.01 to 1
Outputs:
- update: float32 [2, 4096, 10240], P(None, 'row', 'col')
- new_rows: float32 [2, 4096], P(None, 'row')
- new_cols: float32 [2, 10240], P(None, 'col')
The draws below stay inside these ranges and needn't reach their ends.
Inputs may be any that keep to these rules, and one draw needn't show every extreme that they name: `grad_terms`: partial gradient terms of the 16 batch shards.
All inputs are finite; a program needn't handle non-finite values.
Results may differ from the reference program's by a relative error of at most 0.0003.
Values sent between devices are 32-bit elements; how exact they have to be, the bound alone decides.
A program may use at most 256 MiB of HBM per device.

```python
import math
import jax
import jax.numpy as jnp
from jax import lax

D = 4096
FF = 10240
MATS = 2
SOURCES = 16


def draw_grad_terms(key, part):
    subkeys = jax.random.split(key, 4)
    full_shape = (SOURCES, MATS, D, FF)
    chosen = jax.random.randint(subkeys[0], (), 0, MATS)
    factor = jnp.where(jnp.arange(MATS) == chosen, 1.0, 0.05).astype(jnp.float32)
    row_scale = jnp.exp(jax.random.uniform(subkeys[1], (MATS, D, 1), jnp.float32, jnp.log(0.3), jnp.log(3.0)))
    col_scale = jnp.exp(jax.random.uniform(subkeys[2], (MATS, 1, FF), jnp.float32, jnp.log(0.3), jnp.log(3.0)))
    base_values = 0.25 * jax.random.truncated_normal(subkeys[3], -4.0, 4.0, full_shape, jnp.float32)
    values = base_values * row_scale[None] * col_scale[None] * factor[None, :, None, None]
    return values.astype(jnp.bfloat16)


def draw_row_moment(key, part):
    subkeys = jax.random.split(jax.random.fold_in(key, 17), 1)
    position = jnp.arange(D, dtype=jnp.float32)[None, :] / jnp.float32(D - 1)
    rough = jnp.exp(jax.random.uniform(subkeys[0], (MATS, D), jnp.float32, jnp.log(0.02), jnp.log(0.2)))
    rising = jnp.exp(position * jnp.log(10.0))
    return (rough * rising).astype(jnp.float32)


def levels(rng, extent, pieces, smallest, top_value):
    def one(dim, shards_of):
        draws = jax.random.uniform(jax.random.fold_in(jax.random.fold_in(rng, 6), dim), (shards_of,), jnp.float32, smallest / len(pieces), top_value / len(pieces))
        return jnp.repeat(jnp.exp(draws), extent[dim] // shards_of).reshape((-1,) + (1,) * (len(extent) - dim - 1))

    gain = one(*pieces[0])
    for cut in pieces[1:]:
        gain = gain * one(*cut)
    return gain


def setup_inputs(seed: int = 0) -> dict:
    keys = jax.random.split(jax.random.key(seed), 4)
    grad_terms = draw_grad_terms(jax.random.fold_in(keys[3], 71), 0)
    row_moment = draw_row_moment(jax.random.fold_in(keys[3], 71), 0)
    col_moment = jnp.clip(jnp.exp(math.log(1.0) - 4.6051702 * jax.random.uniform(keys[2], (MATS, FF), jnp.float32) ** levels(keys[2], (MATS, FF), ((1, 16),), -0.2, 0.2)), 0.01, 1.0)
    return dict(grad_terms=grad_terms, row_moment=row_moment, col_moment=col_moment)


second_decay = 1.0 - 100.0 ** (-0.8)
tiny_square = 1e-30

def reference(grad_terms, row_moment, col_moment):

    def accumulate(source, running):
        return running + grad_terms[source].astype(jnp.float32)
    gradient = lax.fori_loop(0, grad_terms.shape[0], accumulate, jnp.zeros(grad_terms.shape[1:], jnp.float32))
    squares = gradient * gradient + tiny_square
    new_rows = second_decay * row_moment + (1.0 - second_decay) * lax.optimization_barrier(jnp.sum(squares, axis=2)) / FF
    new_cols = second_decay * col_moment + (1.0 - second_decay) * lax.optimization_barrier(jnp.sum(squares, axis=1)) / D
    row_level = lax.optimization_barrier(jnp.sum(new_rows, axis=1)) / D
    estimate = new_rows[:, :, None] * new_cols[:, None, :] / row_level[:, None, None]
    raw_update = gradient / jnp.sqrt(estimate)
    clip_scale = jnp.maximum(1.0, jnp.sqrt(lax.optimization_barrier(jnp.sum(raw_update * raw_update, axis=(1, 2))) / (D * FF)))
    update = raw_update / clip_scale[:, None, None]
    return (update, new_rows, new_cols)
```

```python
import functools

import jax
import jax.numpy as jnp
from jax import lax
from jax.experimental import pallas as pl
from jax.experimental.pallas import tpu as pltpu
from jax.sharding import Mesh
from jax.sharding import PartitionSpec as P

MESH = pl.DeviceIdType.MESH
COL = ("col_0", "col_1")
ROW = ("row_0", "row_1")
RING = 4
LANES = 128
HALF = 8
CHUNK = 2 * HALF
X_SLOTS = 6
X_AHEAD = 3
S_SLOTS = 4

second_decay = 1.0 - 100.0 ** (-0.8)
tiny_square = 1e-30


def wait_bytes(ref, sem):
    pltpu.make_async_copy(ref, ref, sem).wait()


def kernel(
    grad_hbm,
    row_moment,
    col_moment,
    update,
    new_rows,
    new_cols,
    x_in,
    stage,
    land1,
    sum1,
    land2,
    sum2,
    grad,
    row_part,
    col_part,
    row_scale,
    row_land,
    col_land,
    all_land,
    fin_land,
    x_sem,
    send0,
    send1,
    send2,
    send3,
    recv1,
    recv2,
    recv3,
    recv4,
    stat_send,
    stat_recv,
):
    mats, rows = row_moment.shape
    width = col_moment.shape[1]
    block = RING * width
    row_groups = rows // LANES
    n_row0, n_row1 = lax.axis_size("row_0"), lax.axis_size("row_1")
    n_row, n_col = n_row0 * n_row1, RING * RING
    total_rows = n_row * rows
    total_cols = n_col * width
    per_mat = rows // (2 * CHUNK)
    chunks = mats * per_mat

    here = (lax.axis_index("col_0"), lax.axis_index("col_1"))
    my_col = here[0] * RING + here[1]
    my_row = lax.axis_index("row_0") * n_row1 + lax.axis_index("row_1")

    def at(axis, step):
        return lax.rem(here[axis] + (step + RING), RING)

    def neighbour(axis, step):
        return {COL[axis]: at(axis, step)}

    def col_peer(d):
        t = lax.rem(my_col + d, n_col)
        return {"col_0": t // RING, "col_1": lax.rem(t, RING)}

    def row_peer(d):
        t = lax.rem(my_row + d, n_row)
        return {"row_0": t // n_row1, "row_1": lax.rem(t, n_row1)}

    def send(src, dst, s_sem, r_sem, device):
        pltpu.make_async_remote_copy(
            src_ref=src,
            dst_ref=dst,
            send_sem=s_sem,
            recv_sem=r_sem,
            device_id=device,
            device_id_type=MESH,
        ).start()

    def load(k):
        slot = lax.rem(k, X_SLOTS)
        m = k // per_mat
        r = pl.multiple_of(lax.rem(k, per_mat) * (2 * CHUNK), 2 * CHUNK)
        return pltpu.make_async_copy(
            grad_hbm.at[0, m, pl.ds(r, 2 * CHUNK), :], x_in.at[slot], x_sem.at[slot]
        )

    def own(color, k, idx, seg):
        outer, inner = (idx, seg) if color == 0 else (seg, idx)
        c = pl.multiple_of(outer * block + inner * width, LANES)
        v = x_in[
            lax.rem(k, X_SLOTS), color * CHUNK : (color + 1) * CHUNK, pl.ds(c, width)
        ]
        v = v.astype(jnp.float32)
        return v[:HALF], v[HALF:]

    def cols(s):
        return slice(s * width, (s + 1) * width)

    def inner_cols(idx):
        return pl.ds(pl.multiple_of(idx * width, LANES), width)

    def prepare(k):
        slot = lax.rem(k, S_SLOTS)
        load(k).wait()
        for color in range(2):

            @pl.when(k >= S_SLOTS)
            def _():
                wait_bytes(stage.at[slot, color], send0.at[slot, color])

            axis = color
            for s in range(RING):
                top, low = own(color, k, at(axis, 2), s)
                stage[slot, color, 0, :, cols(s)] = top
                stage[slot, color, 1, :, cols(s)] = low
            for s in range(RING):
                _, low = own(color, k, at(axis, 1), s)
                stage[slot, color, 2, :, cols(s)] = low
                top, _ = own(color, k, at(axis, -1), s)
                stage[slot, color, 3, :, cols(s)] = top

    def stage0(k):
        slot = lax.rem(k, S_SLOTS)
        for which, step, land in ((0, 1, 0), (1, -1, 1)):
            for color in range(2):
                send(
                    stage.at[slot, color, which],
                    land1.at[k, color, land],
                    send0.at[slot, color],
                    recv1.at[k, color],
                    neighbour(color, step),
                )
        for which, step in ((2, 1), (3, -1)):
            for color in range(2):
                send(
                    stage.at[slot, color, which],
                    sum1.at[k, color, which],
                    send0.at[slot, color],
                    recv2.at[k, color],
                    neighbour(color, step),
                )

    def stage1(k):
        slot = lax.rem(k, S_SLOTS)
        for color in range(2):
            axis = color
            wait_bytes(land1.at[k, color], recv1.at[k, color])

            @pl.when(k >= S_SLOTS)
            def _():
                wait_bytes(land1.at[k, color], send1.at[slot, color])

            for s in range(RING):
                top, _ = own(color, k, at(axis, 1), s)
                land1[k, color, 0, :, cols(s)] = land1[k, color, 0, :, cols(s)] + top
                _, low = own(color, k, at(axis, -1), s)
                land1[k, color, 1, :, cols(s)] = land1[k, color, 1, :, cols(s)] + low
            for which, step in ((0, 1), (1, -1)):
                send(
                    land1.at[k, color, which],
                    sum1.at[k, color, which],
                    send1.at[slot, color],
                    recv2.at[k, color],
                    neighbour(axis, step),
                )

    def stage2(k):
        slot = lax.rem(k, S_SLOTS)
        for color in range(2):
            axis = color
            wait_bytes(sum1.at[k, color], recv2.at[k, color])

            @pl.when(k >= S_SLOTS)
            def _():
                wait_bytes(sum2.at[k, color], send2.at[slot, color])

            for s in range(RING):
                top, low = own(color, k, at(axis, 0), s)
                sum1[k, color, 0, :, cols(s)] = (
                    sum1[k, color, 0, :, cols(s)]
                    + sum1[k, color, 3, :, cols(s)]
                    + top
                )
                sum1[k, color, 1, :, cols(s)] = (
                    sum1[k, color, 1, :, cols(s)]
                    + sum1[k, color, 2, :, cols(s)]
                    + low
                )
            axis = 1 - color
            for which, step in ((0, 1), (1, -1)):
                send(
                    sum1.at[k, color, which, :, inner_cols(at(axis, 2))],
                    land2.at[k, color, which],
                    send2.at[slot, color],
                    recv3.at[k, color],
                    neighbour(axis, step),
                )
            for half, which, step in ((1, 2, 1), (0, 3, -1)):
                send(
                    sum1.at[k, color, half, :, inner_cols(at(axis, step))],
                    sum2.at[k, color, which],
                    send2.at[slot, color],
                    recv4.at[k, color],
                    neighbour(axis, step),
                )

    def stage3(k):
        slot = lax.rem(k, S_SLOTS)
        for color in range(2):
            axis = 1 - color
            wait_bytes(land2.at[k, color], recv3.at[k, color])

            @pl.when(k >= S_SLOTS)
            def _():
                wait_bytes(land2.at[k, color], send3.at[slot, color])

            for which, step in ((0, 1), (1, -1)):
                land2[k, color, which] = (
                    land2[k, color, which]
                    + sum1[k, color, which, :, inner_cols(at(axis, step))]
                )
                send(
                    land2.at[k, color, which],
                    sum2.at[k, color, which],
                    send3.at[slot, color],
                    recv4.at[k, color],
                    neighbour(axis, step),
                )

    def lane_tiles(v):
        out = v[:, :LANES]
        for c in range(1, width // LANES):
            out = out + v[:, c * LANES : (c + 1) * LANES]
        return out

    def stage4(k):
        m = k // per_mat
        r = lax.rem(k, per_mat) * (2 * CHUNK)
        squares_sum = col_part[m]
        for color in range(2):
            axis = 1 - color
            wait_bytes(sum2.at[k, color], recv4.at[k, color])
            for half, other in ((0, 3), (1, 2)):
                g = (
                    sum2[k, color, half]
                    + sum2[k, color, other]
                    + sum1[k, color, half, :, inner_cols(at(axis, 0))]
                )
                here_rows = pl.ds(
                    pl.multiple_of(r + color * CHUNK + half * HALF, HALF), HALF
                )
                grad[m, here_rows, :] = g
                squares = g * g + tiny_square
                row_part[m, here_rows, :] = lane_tiles(squares)
                squares_sum = squares_sum + squares
        col_part[m] = squares_sum

    def pick(ref, m, lanes):
        return jnp.where(m == 0, ref[0:1, lanes], ref[1:2, lanes])

    def put(ref, m, lanes, value):
        for i in range(mats):

            @pl.when(m == i)
            def _():
                ref[i : i + 1, lanes] = value

    def all_cols(m, buf, which):
        mine = buf.at[m, my_col]

        def one(d, _):
            send(mine, mine, stat_send.at[m, which], stat_recv.at[m, which], col_peer(d))
            return 0

        lax.fori_loop(1, n_col, one, 0)

    def all_rows(m, buf, which):
        mine = buf.at[m, my_row]

        def one(d, _):
            send(mine, mine, stat_send.at[m, which], stat_recv.at[m, which], row_peer(d))
            return 0

        lax.fori_loop(1, n_row, one, 0)

    def wait_all(m, buf, which, n):
        if n > 1:
            wait_bytes(buf.at[m, pl.ds(0, n - 1)], stat_recv.at[m, which])

    def wait_sent(m, buf, which, n):
        if n > 1:
            wait_bytes(buf.at[m, pl.ds(0, n - 1)], stat_send.at[m, which])

    def statistics1(m):
        for b in range(row_groups):
            part = row_part[m, b * LANES : (b + 1) * LANES, :]
            row_land[m, my_col, b : b + 1, :] = jnp.sum(part.T, axis=0, keepdims=True)
        col_land[m, my_row] = jnp.sum(col_part[m], axis=0, keepdims=True)
        all_cols(m, row_land, 0)
        all_rows(m, col_land, 1)

    def statistics2(m):
        wait_all(m, row_land, 0, n_col)
        wait_all(m, col_land, 1, n_row)
        full = row_land[m, 0]
        for s in range(1, n_col):
            full = full + row_land[m, s]
        moments = []
        for b in range(row_groups):
            moment = (
                second_decay * pick(row_moment, m, slice(b * LANES, (b + 1) * LANES))
                + (1.0 - second_decay) * full[b : b + 1] / total_cols
            )
            put(new_rows, m, slice(b * LANES, (b + 1) * LANES), moment)
            moments.append(moment)
            row_scale[b * LANES : (b + 1) * LANES, :] = jnp.broadcast_to(
                lax.rsqrt(moment), (LANES, LANES)
            ).T
        full = col_land[m, 0]
        for s in range(1, n_row):
            full = full + col_land[m, s]
        col = (
            second_decay * pick(col_moment, m, slice(None))
            + (1.0 - second_decay) * full / total_rows
        )
        put(new_cols, m, slice(None), col)
        col_scale = jnp.broadcast_to(lax.rsqrt(col), (HALF, width))

        def rescale(t, total):
            r = pl.ds(pl.multiple_of(t * HALF, HALF), HALF)
            scale = row_scale[r, :]
            for c in range(width // LANES):
                lanes = slice(c * LANES, (c + 1) * LANES)
                v = grad[m, r, lanes] * col_scale[:, lanes] * scale
                update[m, r, lanes] = v
                total = total + v * v
            return total

        total = lax.fori_loop(
            0, rows // HALF, rescale, jnp.zeros((HALF, LANES), jnp.float32)
        )
        level = moments[0]
        for moment in moments[1:]:
            level = level + moment
        all_land[m, my_col] = total
        fin_land[m, my_row, HALF : HALF + 1, :] = level
        all_cols(m, all_land, 2)

    def statistics3(m):
        wait_all(m, all_land, 2, n_col)
        total = all_land[m, 0]
        for s in range(1, n_col):
            total = total + all_land[m, s]
        fin_land[m, my_row, :HALF, :] = total
        all_rows(m, fin_land, 3)

    def statistics4(m):
        wait_all(m, fin_land, 3, n_row)
        total = fin_land[m, 0]
        for s in range(1, n_row):
            total = total + fin_land[m, s]
        level = jnp.sum(total[HALF : HALF + 1], axis=1, keepdims=True) / total_rows
        clip = jnp.sum(
            jnp.sum(total[:HALF], axis=0, keepdims=True), axis=1, keepdims=True
        )
        clip_scale = jnp.maximum(
            1.0, jnp.sqrt(clip * level / (total_rows * total_cols))
        )
        factor = jnp.broadcast_to(jnp.sqrt(level) / clip_scale, (HALF, width))

        def finish(t, _):
            r = pl.ds(pl.multiple_of(t * HALF, HALF), HALF)
            update[m, r, :] = update[m, r, :] * factor
            return 0

        lax.fori_loop(0, rows // HALF, finish, 0)
        wait_sent(m, row_land, 0, n_col)
        wait_sent(m, col_land, 1, n_row)
        wait_sent(m, all_land, 2, n_col)
        wait_sent(m, fin_land, 3, n_row)

    barrier = pltpu.get_barrier_semaphore()

    def greet_col(d, _):
        pl.semaphore_signal(
            barrier, inc=1, device_id=col_peer(d), device_id_type=MESH
        )
        return 0

    def greet_row(d, _):
        pl.semaphore_signal(
            barrier, inc=1, device_id=row_peer(d), device_id_type=MESH
        )
        return 0

    for k in range(X_AHEAD):
        load(k).start()
    lax.fori_loop(1, n_col, greet_col, 0)
    lax.fori_loop(1, n_row, greet_row, 0)
    col_part[...] = jnp.zeros_like(col_part)
    fin_land[...] = jnp.zeros_like(fin_land)
    prepare(0)
    pl.semaphore_wait(barrier, n_col - 1 + n_row - 1)

    def step(it, _):
        @pl.when(it < chunks)
        def _():
            stage0(it)

            @pl.when(it + X_AHEAD < chunks)
            def _():
                load(it + X_AHEAD).start()

        for lag, work in ((1, stage1), (2, stage2), (3, stage3), (4, stage4)):

            @pl.when((it >= lag) & (it < chunks + lag))
            def _():
                work(it - lag)

        @pl.when(it + 1 < chunks)
        def _():
            prepare(it + 1)

        for when, work in (
            ((per_mat + 3, chunks + 3), statistics1),
            ((per_mat + 5, chunks + 4), statistics2),
            ((per_mat + 7, chunks + 5), statistics3),
            ((per_mat + 9, chunks + 6), statistics4),
        ):

            @pl.when((it == when[0]) | (it == when[1]))
            def _():
                work(jnp.where(it == when[0], 0, 1))

        return 0

    lax.fori_loop(0, chunks + 7, step, 0)

    def drain(slot, _):
        for color in range(2):
            wait_bytes(stage.at[slot, color], send0.at[slot, color])
            wait_bytes(land1.at[0, color], send1.at[slot, color])
            wait_bytes(sum2.at[0, color], send2.at[slot, color])
            wait_bytes(land2.at[0, color], send3.at[slot, color])
        return 0

    lax.fori_loop(0, S_SLOTS, drain, 0)


def on_device(grad_terms, row_moment, col_moment):
    _, mats, rows, _ = grad_terms.shape
    width = col_moment.shape[1]
    n_row = lax.axis_size("row_0") * lax.axis_size("row_1")
    n_col = RING * RING
    chunks = mats * rows // (2 * CHUNK)
    f32 = jnp.float32
    vmem = pl.BlockSpec(memory_space=pltpu.VMEM)
    dma = pltpu.SemaphoreType.DMA
    return pl.pallas_call(
        kernel,
        out_shape=(
            jax.ShapeDtypeStruct((mats, rows, width), f32),
            jax.ShapeDtypeStruct((mats, rows), f32),
            jax.ShapeDtypeStruct((mats, width), f32),
        ),
        in_specs=[pl.BlockSpec(memory_space=pl.ANY), vmem, vmem],
        out_specs=(vmem, vmem, vmem),
        scratch_shapes=[
            pltpu.VMEM((X_SLOTS, 2 * CHUNK, n_col * width), jnp.bfloat16),
            pltpu.VMEM((S_SLOTS, 2, 4, HALF, RING * width), f32),
            pltpu.VMEM((chunks, 2, 2, HALF, RING * width), f32),
            pltpu.VMEM((chunks, 2, 4, HALF, RING * width), f32),
            pltpu.VMEM((chunks, 2, 2, HALF, width), f32),
            pltpu.VMEM((chunks, 2, 4, HALF, width), f32),
            pltpu.VMEM((mats, rows, width), f32),
            pltpu.VMEM((mats, rows, LANES), f32),
            pltpu.VMEM((mats, HALF, width), f32),
            pltpu.VMEM((rows, LANES), f32),
            pltpu.VMEM((mats, n_col, rows // LANES, LANES), f32),
            pltpu.VMEM((mats, n_row, 1, width), f32),
            pltpu.VMEM((mats, n_col, HALF, LANES), f32),
            pltpu.VMEM((mats, n_row, 2 * HALF, LANES), f32),
            dma((X_SLOTS,)),
            dma((S_SLOTS, 2)),
            dma((S_SLOTS, 2)),
            dma((S_SLOTS, 2)),
            dma((S_SLOTS, 2)),
            dma((chunks, 2)),
            dma((chunks, 2)),
            dma((chunks, 2)),
            dma((chunks, 2)),
            dma((mats, 4)),
            dma((mats, 4)),
        ],
        compiler_params=pltpu.CompilerParams(
            collective_id=0,
            has_side_effects=True,
            vmem_limit_bytes=60 * 1024 * 1024,
        ),
    )(grad_terms, row_moment, col_moment)


def solution(mesh):
    n_row = mesh.shape["row"]
    core = 2 if n_row > 1 else 1
    torus = Mesh(
        mesh.devices.reshape(n_row // core, core, RING, RING), ROW + COL
    )
    in_specs = (P(COL, None, ROW, None), P(None, ROW), P(None, COL))
    out_specs = (P(None, ROW, COL), P(None, ROW), P(None, COL))
    return jax.shard_map(
        on_device, mesh=torus, in_specs=in_specs, out_specs=out_specs, check_vma=False
    )
```

```python
import functools

import jax
import jax.numpy as jnp
from jax import lax
from jax.experimental import pallas as pl
from jax.experimental.pallas import tpu as pltpu
from jax.sharding import Mesh
from jax.sharding import PartitionSpec as P

MESH = pl.DeviceIdType.MESH
COL = ("col_0", "col_1")
ROW = ("row_0", "row_1")
RING = 4
LANES = 128
HALF = 16
CHUNK = 2 * HALF
X_SLOTS = 5
X_AHEAD = 2
S_SLOTS = 3
TILE = 8
LAGS = (1, 2, 3, 4)

second_decay = 1.0 - 100.0 ** (-0.8)
tiny_square = 1e-30


def far_first(n_z, n_core):
    def hops(step, n):
        return min(step, n - step)

    steps = [
        (z, core, x, y)
        for z in range(n_z)
        for core in range(n_core)
        for x in range(RING)
        for y in range(RING)
    ]
    steps.sort(
        key=lambda s: -(hops(s[0], n_z) + hops(s[2], RING) + hops(s[3], RING))
    )
    return [s for s in steps if any(s)]


def wait_bytes(ref, sem):
    pltpu.make_async_copy(ref, ref, sem).wait()


def kernel(
    grad_hbm,
    row_hbm,
    col_hbm,
    update,
    factor,
    new_rows,
    new_cols,
    x_in,
    stage,
    land1,
    sum1,
    land2,
    sum2,
    row_moment,
    col_moment,
    row_part,
    col_part,
    weighted,
    weighted_row,
    row_scale,
    row_land,
    col_land,
    all_land,
    x_sem,
    m_sem,
    send0,
    send1,
    send2,
    send3,
    recv1,
    recv2,
    recv3,
    recv4,
    stat_send,
    stat_recv,
):
    mats, rows = row_moment.shape
    offsets = far_first(lax.axis_size("row_0"), lax.axis_size("row_1"))
    width = col_moment.shape[1]
    block = RING * width
    row_groups = rows // LANES
    n_row0, n_row1 = lax.axis_size("row_0"), lax.axis_size("row_1")
    n_row, n_col = n_row0 * n_row1, RING * RING
    total_rows = n_row * rows
    total_cols = n_col * width
    per_mat = rows // (2 * CHUNK)
    chunks = mats * per_mat

    here = (lax.axis_index("col_0"), lax.axis_index("col_1"))
    my_col = here[0] * RING + here[1]
    my_row = lax.axis_index("row_0") * n_row1 + lax.axis_index("row_1")

    def at(axis, step):
        return lax.rem(here[axis] + (step + RING), RING)

    me = my_row * n_col + my_col

    def neighbour(axis, step):
        return {COL[axis]: at(axis, step)}

    def col_peer(d):
        t = lax.rem(my_col + d, n_col)
        return {"col_0": t // RING, "col_1": lax.rem(t, RING)}

    def row_peer(d):
        t = lax.rem(my_row + d, n_row)
        return {"row_0": t // n_row1, "row_1": lax.rem(t, n_row1)}

    def send(src, dst, s_sem, r_sem, device):
        pltpu.make_async_remote_copy(
            src_ref=src,
            dst_ref=dst,
            send_sem=s_sem,
            recv_sem=r_sem,
            device_id=device,
            device_id_type=MESH,
        ).start()

    def load(k):
        slot = lax.rem(k, X_SLOTS)
        m = k // per_mat
        r = pl.multiple_of(lax.rem(k, per_mat) * (2 * CHUNK), 2 * CHUNK)
        return pltpu.make_async_copy(
            grad_hbm.at[0, m, pl.ds(r, 2 * CHUNK), :], x_in.at[slot], x_sem.at[slot]
        )

    def own(color, k, idx, seg):
        outer, inner = (idx, seg) if color == 0 else (seg, idx)
        c = pl.multiple_of(outer * block + inner * width, LANES)
        v = x_in[
            lax.rem(k, X_SLOTS), color * CHUNK : (color + 1) * CHUNK, pl.ds(c, width)
        ]
        v = v.astype(jnp.float32)
        return v[:HALF], v[HALF:]

    def cols(s):
        return slice(s * width, (s + 1) * width)

    def inner_cols(idx):
        return pl.ds(pl.multiple_of(idx * width, LANES), width)

    def prepare(k):
        slot = lax.rem(k, S_SLOTS)
        load(k).wait()
        for color in range(2):

            @pl.when(k >= S_SLOTS)
            def _():
                wait_bytes(stage.at[slot, color], send0.at[slot, color])

            axis = color
            for s in range(RING):
                top, low = own(color, k, at(axis, 2), s)
                stage[slot, color, 0, :, cols(s)] = top
                stage[slot, color, 1, :, cols(s)] = low
            for s in range(RING):
                _, low = own(color, k, at(axis, 1), s)
                stage[slot, color, 2, :, cols(s)] = low
                top, _ = own(color, k, at(axis, -1), s)
                stage[slot, color, 3, :, cols(s)] = top

    def stage0(k):
        slot = lax.rem(k, S_SLOTS)
        for which, step, land in ((0, 1, 0), (1, -1, 1)):
            for color in range(2):
                send(
                    stage.at[slot, color, which],
                    land1.at[k, color, land],
                    send0.at[slot, color],
                    recv1.at[k, color],
                    neighbour(color, step),
                )
        for which, step in ((2, 1), (3, -1)):
            for color in range(2):
                send(
                    stage.at[slot, color, which],
                    sum1.at[k, color, which],
                    send0.at[slot, color],
                    recv2.at[k, color],
                    neighbour(color, step),
                )

    def stage1(k):
        slot = lax.rem(k, S_SLOTS)
        for color in range(2):
            axis = color
            wait_bytes(land1.at[k, color], recv1.at[k, color])

            @pl.when(k >= S_SLOTS)
            def _():
                wait_bytes(land1.at[k, color], send1.at[slot, color])

            for s in range(RING):
                top, _ = own(color, k, at(axis, 1), s)
                land1[k, color, 0, :, cols(s)] = land1[k, color, 0, :, cols(s)] + top
                _, low = own(color, k, at(axis, -1), s)
                land1[k, color, 1, :, cols(s)] = land1[k, color, 1, :, cols(s)] + low
            for which, step in ((0, 1), (1, -1)):
                send(
                    land1.at[k, color, which],
                    sum1.at[k, color, which],
                    send1.at[slot, color],
                    recv2.at[k, color],
                    neighbour(axis, step),
                )

    def stage2(k):
        slot = lax.rem(k, S_SLOTS)
        for color in range(2):
            axis = color
            wait_bytes(sum1.at[k, color], recv2.at[k, color])

            @pl.when(k >= S_SLOTS)
            def _():
                wait_bytes(sum2.at[k, color], send2.at[slot, color])

            for s in range(RING):
                top, low = own(color, k, at(axis, 0), s)
                sum1[k, color, 0, :, cols(s)] = (
                    sum1[k, color, 0, :, cols(s)]
                    + sum1[k, color, 3, :, cols(s)]
                    + top
                )
                sum1[k, color, 1, :, cols(s)] = (
                    sum1[k, color, 1, :, cols(s)]
                    + sum1[k, color, 2, :, cols(s)]
                    + low
                )
            axis = 1 - color
            for which, step in ((0, 1), (1, -1)):
                send(
                    sum1.at[k, color, which, :, inner_cols(at(axis, 2))],
                    land2.at[k, color, which],
                    send2.at[slot, color],
                    recv3.at[k, color],
                    neighbour(axis, step),
                )
            for half, which, step in ((1, 2, 1), (0, 3, -1)):
                send(
                    sum1.at[k, color, half, :, inner_cols(at(axis, step))],
                    sum2.at[k, color, which],
                    send2.at[slot, color],
                    recv4.at[k, color],
                    neighbour(axis, step),
                )

    def stage3(k):
        slot = lax.rem(k, S_SLOTS)
        for color in range(2):
            axis = 1 - color
            wait_bytes(land2.at[k, color], recv3.at[k, color])

            @pl.when(k >= S_SLOTS)
            def _():
                wait_bytes(land2.at[k, color], send3.at[slot, color])

            for which, step in ((0, 1), (1, -1)):
                land2[k, color, which] = (
                    land2[k, color, which]
                    + sum1[k, color, which, :, inner_cols(at(axis, step))]
                )
                send(
                    land2.at[k, color, which],
                    sum2.at[k, color, which],
                    send3.at[slot, color],
                    recv4.at[k, color],
                    neighbour(axis, step),
                )

    def lane_tiles(v):
        out = v[:, :LANES]
        for c in range(1, width // LANES):
            out = out + v[:, c * LANES : (c + 1) * LANES]
        return out

    def stage4(k):
        m = k // per_mat
        r = lax.rem(k, per_mat) * (2 * CHUNK)
        squares_sum = col_part[m]
        for color in range(2):
            axis = 1 - color
            wait_bytes(sum2.at[k, color], recv4.at[k, color])
            for half, other in ((0, 3), (1, 2)):
                g = (
                    sum2[k, color, half]
                    + sum2[k, color, other]
                    + sum1[k, color, half, :, inner_cols(at(axis, 0))]
                )
                here_rows = pl.ds(
                    pl.multiple_of(r + color * CHUNK + half * HALF, HALF), HALF
                )
                update[m, here_rows, :] = g
                squares = g * g + tiny_square
                row_part[m, here_rows, :] = lane_tiles(squares)
                for t in range(HALF // TILE):
                    squares_sum = squares_sum + squares[t * TILE : (t + 1) * TILE]
        col_part[m] = squares_sum

    def pick(ref, m, lanes):
        return jnp.where(m == 0, ref[0:1, lanes], ref[1:2, lanes])

    def put(ref, m, lanes, value):
        for i in range(mats):

            @pl.when(m == i)
            def _():
                ref[i : i + 1, lanes] = value

    def lane_major(part):
        return jnp.sum(part.T, axis=0, keepdims=True)

    def group(b):
        return slice(b * LANES, (b + 1) * LANES)

    def share_sums(m):
        for b in range(row_groups):
            row_land[m, my_col, b : b + 1, :] = lane_major(row_part[m, group(b), :])
        col_land[m, my_row] = jnp.sum(col_part[m], axis=0, keepdims=True)
        mine = col_land.at[m, my_row]

        def to_row(d, _):
            send(mine, mine, stat_send.at[m, 0], stat_recv.at[m, 0], row_peer(d))
            return 0

        lax.fori_loop(1, n_row, to_row, 0)
        rows_mine = row_land.at[m, my_col]

        def to_col(d, _):
            send(
                rows_mine, rows_mine, stat_send.at[m, 1], stat_recv.at[m, 1], col_peer(d)
            )
            return 0

        lax.fori_loop(1, n_col, to_col, 0)

    def all_but_one(m, buf, sem, n):
        if n > 1:
            wait_bytes(buf.at[m, pl.ds(0, n - 1)], sem)

    def share_clip(m):
        all_but_one(m, col_land, stat_recv.at[m, 0], n_row)
        full = col_land[m, 0]
        for s in range(1, n_row):
            full = full + col_land[m, s]
        col = (
            second_decay * pick(col_moment, m, slice(None))
            + (1.0 - second_decay) * full / total_rows
        )
        put(new_cols, m, slice(None), col)
        inverse = jnp.broadcast_to(1.0 / col, (TILE, width))

        def weigh(t, _):
            r = pl.ds(pl.multiple_of(t * TILE, TILE), TILE)
            v = update[m, r, :]
            weighted[r, :] = lane_tiles(v * v * inverse)
            return 0

        lax.fori_loop(0, rows // TILE, weigh, 0)
        for b in range(row_groups):
            weighted_row[b : b + 1, :] = lane_major(weighted[group(b), :])

        all_but_one(m, row_land, stat_recv.at[m, 1], n_col)
        full = row_land[m, 0]
        for s in range(1, n_col):
            full = full + row_land[m, s]
        moments, clip, level = [], None, None
        for b in range(row_groups):
            moment = (
                second_decay * pick(row_moment, m, group(b))
                + (1.0 - second_decay) * full[b : b + 1] / total_cols
            )
            part = weighted_row[b : b + 1, :] / moment
            clip = part if clip is None else clip + part
            level = moment if level is None else level + moment
            moments.append(moment)
        all_land[m, me, 0:1, :] = clip
        all_land[m, me, 1:2, :] = level
        mine = all_land.at[m, me]
        for step in offsets:
            z, core, x, y = step
            there = {
                "row_0": lax.rem(lax.axis_index("row_0") + z, n_row0),
                "row_1": lax.rem(lax.axis_index("row_1") + core, n_row1),
                "col_0": at(0, x),
                "col_1": at(1, y),
            }
            send(mine, mine, stat_send.at[m, 2], stat_recv.at[m, 2], there)
        for b in range(row_groups):
            put(new_rows, m, group(b), moments[b])
            row_scale[group(b), :] = jnp.broadcast_to(
                lax.rsqrt(moments[b]), (LANES, LANES)
            ).T
        col_scale = jnp.broadcast_to(lax.rsqrt(col), (TILE, width))

        def rescale(t, _):
            r = pl.ds(pl.multiple_of(t * TILE, TILE), TILE)
            scale = row_scale[r, :]
            for c in range(width // LANES):
                lanes = group(c)
                update[m, r, lanes] = update[m, r, lanes] * col_scale[:, lanes] * scale
            return 0

        lax.fori_loop(0, rows // TILE, rescale, 0)

    def finish(m):
        all_but_one(m, all_land, stat_recv.at[m, 2], n_row * n_col)
        total = jnp.sum(all_land[m], axis=0)
        level = jnp.sum(total[1:2], axis=1, keepdims=True) / (n_col * total_rows)
        clip = jnp.sum(total[0:1], axis=1, keepdims=True)
        clip_scale = jnp.maximum(
            1.0, jnp.sqrt(clip * level / (total_rows * total_cols))
        )
        scale = jnp.broadcast_to(jnp.sqrt(level) / clip_scale, (TILE, LANES))
        factor[m] = scale
        all_but_one(m, col_land, stat_send.at[m, 0], n_row)
        all_but_one(m, row_land, stat_send.at[m, 1], n_col)
        all_but_one(m, all_land, stat_send.at[m, 2], n_row * n_col)

    barrier = pltpu.get_barrier_semaphore()
    row_copy = pltpu.make_async_copy(row_hbm, row_moment, m_sem.at[0])
    col_copy = pltpu.make_async_copy(col_hbm, col_moment, m_sem.at[1])

    def greet_row(d, _):
        pl.semaphore_signal(
            barrier, inc=1, device_id=row_peer(d), device_id_type=MESH
        )
        return 0

    for k in range(X_AHEAD):
        load(k).start()
    for axis in range(2):
        for to in (1, -1):
            pl.semaphore_signal(
                barrier, inc=1, device_id=neighbour(axis, to), device_id_type=MESH
            )
    lax.fori_loop(1, n_row, greet_row, 0)
    col_part[...] = jnp.zeros_like(col_part)
    row_copy.start()
    col_copy.start()
    prepare(0)
    pl.semaphore_wait(barrier, 4 + n_row - 1)
    row_copy.wait()
    col_copy.wait()

    def step(it, _):
        @pl.when(it < chunks)
        def _():
            stage0(it)

            @pl.when(it + X_AHEAD < chunks)
            def _():
                load(it + X_AHEAD).start()

        for lag, work in zip(LAGS, (stage1, stage2, stage3, stage4)):

            @pl.when((it >= lag) & (it < chunks + lag))
            def _():
                work(it - lag)

        @pl.when(it + 1 < chunks)
        def _():
            prepare(it + 1)

        for when, work in (
            ((per_mat - 1 + LAGS[3], chunks - 1 + LAGS[3]), share_sums),
            ((per_mat + 1 + LAGS[3], chunks + LAGS[3]), share_clip),
            ((per_mat + 3 + LAGS[3], chunks + 1 + LAGS[3]), finish),
        ):

            @pl.when((it == when[0]) | (it == when[1]))
            def _():
                work(jnp.where(it == when[0], 0, 1))

        return 0

    lax.fori_loop(0, chunks + 2 + LAGS[3], step, 0)

    def drain(slot, _):
        for color in range(2):
            wait_bytes(stage.at[slot, color], send0.at[slot, color])
            wait_bytes(land1.at[0, color], send1.at[slot, color])
            wait_bytes(sum2.at[0, color], send2.at[slot, color])
            wait_bytes(land2.at[0, color], send3.at[slot, color])
        return 0

    lax.fori_loop(0, S_SLOTS, drain, 0)


def finish_kernel(
    scaled, factor, new_rows, new_cols, update_hbm, rows_hbm, cols_hbm, out, sems
):
    mats, rows, width = scaled.shape
    pieces = 4
    copies = [
        pltpu.make_async_copy(new_rows, rows_hbm, sems.at[0]),
        pltpu.make_async_copy(new_cols, cols_hbm, sems.at[1]),
    ]
    for copy in copies:
        copy.start()
    size = rows // pieces
    for m in range(mats):
        scale = jnp.broadcast_to(factor[m][:, :1], (TILE, width))
        for p in range(pieces):

            def one(t, _):
                r = pl.ds(pl.multiple_of(p * size + t * TILE, TILE), TILE)
                out[m, r, :] = scaled[m, r, :] * scale
                return 0

            lax.fori_loop(0, size // TILE, one, 0, unroll=True)
            here = pl.ds(p * size, size)
            copy = pltpu.make_async_copy(
                out.at[m, here], update_hbm.at[m, here], sems.at[2 + m * pieces + p]
            )
            copy.start()
            copies.append(copy)
    for copy in copies:
        copy.wait()


def on_device(grad_terms, row_moment, col_moment):
    _, mats, rows, _ = grad_terms.shape
    width = col_moment.shape[1]
    n_row = lax.axis_size("row_0") * lax.axis_size("row_1")
    n_col = RING * RING
    chunks = mats * rows // (2 * CHUNK)
    f32 = jnp.float32
    vmem = pl.BlockSpec(memory_space=pltpu.VMEM)
    hbm = pl.BlockSpec(memory_space=pltpu.HBM)
    dma = pltpu.SemaphoreType.DMA
    shapes = (
        jax.ShapeDtypeStruct((mats, rows, width), f32),
        jax.ShapeDtypeStruct((mats, TILE, LANES), f32),
        jax.ShapeDtypeStruct((mats, rows), f32),
        jax.ShapeDtypeStruct((mats, width), f32),
    )
    scaled, factor, new_rows, new_cols = pl.pallas_call(
        kernel,
        out_shape=shapes,
        in_specs=[hbm, hbm, hbm],
        out_specs=(vmem, vmem, vmem, vmem),
        scratch_shapes=[
            pltpu.VMEM((X_SLOTS, 2 * CHUNK, n_col * width), jnp.bfloat16),
            pltpu.VMEM((S_SLOTS, 2, 4, HALF, RING * width), f32),
            pltpu.VMEM((chunks, 2, 2, HALF, RING * width), f32),
            pltpu.VMEM((chunks, 2, 4, HALF, RING * width), f32),
            pltpu.VMEM((chunks, 2, 2, HALF, width), f32),
            pltpu.VMEM((chunks, 2, 4, HALF, width), f32),
            pltpu.VMEM((mats, rows), f32),
            pltpu.VMEM((mats, width), f32),
            pltpu.VMEM((mats, rows, LANES), f32),
            pltpu.VMEM((mats, TILE, width), f32),
            pltpu.VMEM((rows, LANES), f32),
            pltpu.VMEM((rows // LANES, LANES), f32),
            pltpu.VMEM((rows, LANES), f32),
            pltpu.VMEM((mats, n_col, rows // LANES, LANES), f32),
            pltpu.VMEM((mats, n_row, 1, width), f32),
            pltpu.VMEM((mats, n_row * n_col, 2, LANES), f32),
            dma((X_SLOTS,)),
            dma((2,)),
            dma((S_SLOTS, 2)),
            dma((S_SLOTS, 2)),
            dma((S_SLOTS, 2)),
            dma((S_SLOTS, 2)),
            dma((chunks, 2)),
            dma((chunks, 2)),
            dma((chunks, 2)),
            dma((chunks, 2)),
            dma((mats, 3)),
            dma((mats, 3)),
        ],
        compiler_params=pltpu.CompilerParams(
            collective_id=0,
            has_side_effects=True,
            vmem_limit_bytes=50 * 1024 * 1024,
        ),
    )(grad_terms, row_moment, col_moment)
    return pl.pallas_call(
        finish_kernel,
        out_shape=(shapes[0], shapes[2], shapes[3]),
        in_specs=[vmem] * 4,
        out_specs=(hbm, hbm, hbm),
        scratch_shapes=[pltpu.VMEM((mats, rows, width), f32), dma((10,))],
        compiler_params=pltpu.CompilerParams(vmem_limit_bytes=4 * 1024 * 1024),
    )(scaled, factor, new_rows, new_cols)


def solution(mesh):
    n_row = mesh.shape["row"]
    core = 2 if n_row > 1 else 1
    torus = Mesh(
        mesh.devices.reshape(n_row // core, core, RING, RING), ROW + COL
    )
    in_specs = (P(COL, None, ROW, None), P(None, ROW), P(None, COL))
    out_specs = (P(None, ROW, COL), P(None, ROW), P(None, COL))
    return jax.shard_map(
        on_device, mesh=torus, in_specs=in_specs, out_specs=out_specs, check_vma=False
    )
```

```python
import functools

import jax
import jax.numpy as jnp
from jax import lax
from jax.experimental import pallas as pl
from jax.experimental.pallas import tpu as pltpu
from jax.sharding import Mesh
from jax.sharding import PartitionSpec as P

MESH = pl.DeviceIdType.MESH
COL = ("col_0", "col_1")
ROW = ("row_0", "row_1")
RING = 4
LANES = 128
HALF = 16
CHUNK = 2 * HALF
X_SLOTS = 5
X_AHEAD = 2
S_SLOTS = 3
TILE = 8
R_SLOTS = 6

second_decay = 1.0 - 100.0 ** (-0.8)
tiny_square = 1e-30


def far_first(n_z, n_core):
    def hops(step, n):
        return min(step, n - step)

    steps = [
        (z, core, x, y)
        for z in range(n_z)
        for core in range(n_core)
        for x in range(RING)
        for y in range(RING)
    ]
    steps.sort(
        key=lambda s: -(hops(s[0], n_z) + hops(s[2], RING) + hops(s[3], RING))
    )
    return [s for s in steps if any(s)]


def wait_bytes(ref, sem):
    pltpu.make_async_copy(ref, ref, sem).wait()


def kernel(
    grad_hbm,
    row_hbm,
    col_hbm,
    update,
    factor,
    new_rows,
    new_cols,
    x_in,
    stage,
    land1,
    sum1,
    land2,
    sum2,
    row_moment,
    col_moment,
    row_part,
    col_part,
    weighted,
    weighted_row,
    row_scale,
    row_land,
    col_land,
    all_land,
    x_sem,
    m_sem,
    send0,
    send1,
    send2,
    send3,
    send5,
    recv1,
    recv2,
    recv3,
    recv4,
    stat_send,
    stat_recv,
):
    mats, rows = row_moment.shape
    offsets = far_first(lax.axis_size("row_0"), lax.axis_size("row_1"))
    width = col_moment.shape[1]
    block = RING * width
    row_groups = rows // LANES
    n_row0, n_row1 = lax.axis_size("row_0"), lax.axis_size("row_1")
    n_row, n_col = n_row0 * n_row1, RING * RING
    total_rows = n_row * rows
    total_cols = n_col * width
    per_mat = rows // (2 * CHUNK)
    chunks = mats * per_mat

    here = (lax.axis_index("col_0"), lax.axis_index("col_1"))
    my_col = here[0] * RING + here[1]
    my_row = lax.axis_index("row_0") * n_row1 + lax.axis_index("row_1")

    def at(axis, step):
        return lax.rem(here[axis] + (step + RING), RING)

    me = my_row * n_col + my_col

    def neighbour(axis, step):
        return {COL[axis]: at(axis, step)}

    def col_peer(d):
        t = lax.rem(my_col + d, n_col)
        return {"col_0": t // RING, "col_1": lax.rem(t, RING)}

    def row_peer(d):
        t = lax.rem(my_row + d, n_row)
        return {"row_0": t // n_row1, "row_1": lax.rem(t, n_row1)}

    def send(src, dst, s_sem, r_sem, device):
        pltpu.make_async_remote_copy(
            src_ref=src,
            dst_ref=dst,
            send_sem=s_sem,
            recv_sem=r_sem,
            device_id=device,
            device_id_type=MESH,
        ).start()

    def load(k, color):
        slot = lax.rem(k, X_SLOTS)
        m = k // per_mat
        r = lax.rem(k, per_mat) * (2 * CHUNK) + color * CHUNK
        return pltpu.make_async_copy(
            grad_hbm.at[0, m, pl.ds(pl.multiple_of(r, CHUNK), CHUNK), :],
            x_in.at[slot, color],
            x_sem.at[slot, color],
        )

    def start_load(k):
        for color in range(2):
            load(k, color).start()

    def own(color, k, idx, seg):
        outer, inner = (idx, seg) if color == 0 else (seg, idx)
        c = pl.multiple_of(outer * block + inner * width, LANES)
        v = x_in[lax.rem(k, X_SLOTS), color, :, pl.ds(c, width)].astype(jnp.float32)
        return v[:HALF], v[HALF:]

    def cols(s):
        return slice(s * width, (s + 1) * width)

    def inner_cols(idx):
        return pl.ds(pl.multiple_of(idx * width, LANES), width)

    def free_stage(k, color):
        slot = lax.rem(k, S_SLOTS)

        @pl.when(k >= S_SLOTS)
        def _():
            wait_bytes(stage.at[slot, color], send0.at[slot, color])

    def prepare_relay(k, color):
        slot = lax.rem(k, S_SLOTS)
        for s in range(RING):
            top, low = own(color, k, at(color, 2), s)
            stage[slot, color, 0, :, cols(s)] = top
            stage[slot, color, 1, :, cols(s)] = low

    def prepare_direct(k, color):
        slot = lax.rem(k, S_SLOTS)
        for s in range(RING):
            _, low = own(color, k, at(color, 1), s)
            stage[slot, color, 2, :, cols(s)] = low
            top, _ = own(color, k, at(color, -1), s)
            stage[slot, color, 3, :, cols(s)] = top

    def prepare(k):
        for color in range(2):
            load(k, color).wait()
            free_stage(k, color)
            prepare_relay(k, color)
            prepare_direct(k, color)

    def send_relay(k, color):
        slot = lax.rem(k, S_SLOTS)
        for which, step in ((0, 1), (1, -1)):
            send(
                stage.at[slot, color, which],
                land1.at[k, color, which],
                send0.at[slot, color],
                recv1.at[lax.rem(k, R_SLOTS), color],
                neighbour(color, step),
            )

    def send_direct(k, color):
        slot = lax.rem(k, S_SLOTS)
        for which, step in ((2, 1), (3, -1)):
            send(
                stage.at[slot, color, which],
                sum1.at[k, color, which],
                send0.at[slot, color],
                recv2.at[lax.rem(k, R_SLOTS), color],
                neighbour(color, step),
            )

    def stage0(k):
        for color in range(2):
            send_relay(k, color)
        for color in range(2):
            send_direct(k, color)

    def stage1(k):
        slot = lax.rem(k, S_SLOTS)
        for color in range(2):
            axis = color
            wait_bytes(land1.at[k, color], recv1.at[lax.rem(k, R_SLOTS), color])

            @pl.when(k >= S_SLOTS)
            def _():
                wait_bytes(land1.at[k, color], send1.at[slot, color])

            for s in range(RING):
                top, _ = own(color, k, at(axis, 1), s)
                land1[k, color, 0, :, cols(s)] = land1[k, color, 0, :, cols(s)] + top
                _, low = own(color, k, at(axis, -1), s)
                land1[k, color, 1, :, cols(s)] = land1[k, color, 1, :, cols(s)] + low
            for which, step in ((0, 1), (1, -1)):
                send(
                    land1.at[k, color, which],
                    sum1.at[k, color, which],
                    send1.at[slot, color],
                    recv2.at[lax.rem(k, R_SLOTS), color],
                    neighbour(axis, step),
                )

    def stage2(k):
        slot = lax.rem(k, S_SLOTS)
        for color in range(2):
            axis = color
            wait_bytes(sum1.at[k, color], recv2.at[lax.rem(k, R_SLOTS), color])

            @pl.when(k >= S_SLOTS)
            def _():
                wait_bytes(land2.at[k, color], send2.at[slot, color])

            for s in range(RING):
                top, low = own(color, k, at(axis, 0), s)
                sum1[k, color, 0, :, cols(s)] = (
                    sum1[k, color, 0, :, cols(s)]
                    + sum1[k, color, 3, :, cols(s)]
                    + top
                )
                sum1[k, color, 1, :, cols(s)] = (
                    sum1[k, color, 1, :, cols(s)]
                    + sum1[k, color, 2, :, cols(s)]
                    + low
                )
            axis = 1 - color
            for which, step in ((0, 1), (1, -1)):
                send(
                    sum1.at[k, color, which, :, inner_cols(at(axis, 2))],
                    land2.at[k, color, which],
                    send2.at[slot, color],
                    recv3.at[lax.rem(k, R_SLOTS), color],
                    neighbour(axis, step),
                )

    def stage2_direct(k):
        slot = lax.rem(k, per_mat)
        for color in range(2):
            axis = 1 - color

            @pl.when(k >= per_mat)
            def _():
                wait_bytes(land2.at[k, color], send5.at[slot, color])

            for half, which, step in ((1, 2, 1), (0, 3, -1)):
                send(
                    sum1.at[k, color, half, :, inner_cols(at(axis, step))],
                    sum2.at[k, color, which],
                    send5.at[slot, color],
                    recv4.at[k, color],
                    neighbour(axis, step),
                )

    def stage3(k):
        slot = lax.rem(k, S_SLOTS)
        for color in range(2):
            axis = 1 - color
            wait_bytes(land2.at[k, color], recv3.at[lax.rem(k, R_SLOTS), color])

            @pl.when(k >= S_SLOTS)
            def _():
                wait_bytes(land2.at[k, color], send3.at[slot, color])

            for which, step in ((0, 1), (1, -1)):
                land2[k, color, which] = (
                    land2[k, color, which]
                    + sum1[k, color, which, :, inner_cols(at(axis, step))]
                )
                send(
                    land2.at[k, color, which],
                    sum2.at[k, color, which],
                    send3.at[slot, color],
                    recv4.at[k, color],
                    neighbour(axis, step),
                )

    def lane_tiles(v):
        out = v[:, :LANES]
        for c in range(1, width // LANES):
            out = out + v[:, c * LANES : (c + 1) * LANES]
        return out

    def stage4(k):
        m = k // per_mat
        r = lax.rem(k, per_mat) * (2 * CHUNK)
        squares_sum = col_part[m]
        for color in range(2):
            axis = 1 - color
            wait_bytes(sum2.at[k, color], recv4.at[k, color])
            for half, other in ((0, 3), (1, 2)):
                g = (
                    sum2[k, color, half]
                    + sum2[k, color, other]
                    + sum1[k, color, half, :, inner_cols(at(axis, 0))]
                )
                here_rows = pl.ds(
                    pl.multiple_of(r + color * CHUNK + half * HALF, HALF), HALF
                )
                update[m, here_rows, :] = g
                squares = g * g + tiny_square
                row_part[m, here_rows, :] = lane_tiles(squares)
                for t in range(HALF // TILE):
                    squares_sum = squares_sum + squares[t * TILE : (t + 1) * TILE]
        col_part[m] = squares_sum

    def pick(ref, m, lanes):
        return jnp.where(m == 0, ref[0:1, lanes], ref[1:2, lanes])

    def put(ref, m, lanes, value):
        for i in range(mats):

            @pl.when(m == i)
            def _():
                ref[i : i + 1, lanes] = value

    def lane_major(part):
        return jnp.sum(part.T, axis=0, keepdims=True)

    def group(b):
        return slice(b * LANES, (b + 1) * LANES)

    def early_sums(m):
        for b in range(row_groups - 1):
            row_land[m, my_col, b : b + 1, :] = lane_major(row_part[m, group(b), :])

    def peer(step):
        z, core, x, y = step
        there = {}
        if z or core:
            there["row_0"] = lax.rem(lax.axis_index("row_0") + z, n_row0)
            there["row_1"] = lax.rem(lax.axis_index("row_1") + core, n_row1)
        if x or y:
            there["col_0"] = at(0, x)
            there["col_1"] = at(1, y)
        return there

    def share_sums(m):
        col_land[m, my_row] = jnp.sum(col_part[m], axis=0, keepdims=True)
        mine = col_land.at[m, my_row]
        for step in offsets:
            if not any(step[2:]):
                send(mine, mine, stat_send.at[m, 0], stat_recv.at[m, 0], peer(step))
        b = row_groups - 1
        row_land[m, my_col, b : b + 1, :] = lane_major(row_part[m, group(b), :])
        rows_mine = row_land.at[m, my_col]
        for step in offsets:
            if not any(step[:2]):
                send(
                    rows_mine,
                    rows_mine,
                    stat_send.at[m, 1],
                    stat_recv.at[m, 1],
                    peer(step),
                )

    def all_but_one(m, buf, sem, n):
        if n > 1:
            wait_bytes(buf.at[m, pl.ds(0, n - 1)], sem)

    def share_clip(m):
        all_but_one(m, col_land, stat_recv.at[m, 0], n_row)
        full = col_land[m, 0]
        for s in range(1, n_row):
            full = full + col_land[m, s]
        col = (
            second_decay * pick(col_moment, m, slice(None))
            + (1.0 - second_decay) * full / total_rows
        )
        inverse = jnp.broadcast_to(1.0 / col, (TILE, width))

        def weigh(t, _):
            r = pl.ds(pl.multiple_of(t * TILE, TILE), TILE)
            v = update[m, r, :]
            weighted[r, :] = lane_tiles(v * v * inverse)
            return 0

        lax.fori_loop(0, rows // TILE, weigh, 0, unroll=8)
        for b in range(row_groups):
            weighted_row[b : b + 1, :] = lane_major(weighted[group(b), :])

        all_but_one(m, row_land, stat_recv.at[m, 1], n_col)
        full = row_land[m, 0]
        for s in range(1, n_col):
            full = full + row_land[m, s]
        moments, clip, level = [], None, None
        for b in range(row_groups):
            moment = (
                second_decay * pick(row_moment, m, group(b))
                + (1.0 - second_decay) * full[b : b + 1] / total_cols
            )
            part = weighted_row[b : b + 1, :] / moment
            clip = part if clip is None else clip + part
            level = moment if level is None else level + moment
            moments.append(moment)
        all_land[m, me, 0:1, :] = clip
        all_land[m, me, 1:2, :] = level
        mine = all_land.at[m, me]
        for step in offsets:
            send(mine, mine, stat_send.at[m, 2], stat_recv.at[m, 2], peer(step))
        put(new_cols, m, slice(None), col)
        for b in range(row_groups):
            put(new_rows, m, group(b), moments[b])
            row_scale[group(b), :] = jnp.broadcast_to(
                lax.rsqrt(moments[b]), (LANES, LANES)
            ).T
        col_scale = jnp.broadcast_to(lax.rsqrt(col), (TILE, width))

        def rescale(t, _):
            r = pl.ds(pl.multiple_of(t * TILE, TILE), TILE)
            scale = row_scale[r, :]
            for c in range(width // LANES):
                lanes = group(c)
                update[m, r, lanes] = update[m, r, lanes] * col_scale[:, lanes] * scale
            return 0

        lax.fori_loop(0, rows // TILE, rescale, 0, unroll=8)

    def finish(m):
        all_but_one(m, all_land, stat_recv.at[m, 2], n_row * n_col)
        parts = [all_land[m, s] for s in range(4)]
        for s in range(4, n_row * n_col):
            parts[s % 4] = parts[s % 4] + all_land[m, s]
        total = (parts[0] + parts[1]) + (parts[2] + parts[3])
        level = jnp.sum(total[1:2], axis=1, keepdims=True) / (n_col * total_rows)
        clip = jnp.sum(total[0:1], axis=1, keepdims=True)
        clip_scale = jnp.maximum(
            1.0, jnp.sqrt(clip * level / (total_rows * total_cols))
        )
        scale = jnp.broadcast_to(jnp.sqrt(level) / clip_scale, (TILE, LANES))
        factor[m] = scale

        @pl.when(m < mats - 1)
        def _():
            wide = jnp.broadcast_to(scale[:, :1], (TILE, width))

            def one(t, _):
                r = pl.ds(pl.multiple_of(t * TILE, TILE), TILE)
                update[m, r, :] = update[m, r, :] * wide
                return 0

            lax.fori_loop(0, rows // TILE, one, 0, unroll=4)

        all_but_one(m, col_land, stat_send.at[m, 0], n_row)
        all_but_one(m, row_land, stat_send.at[m, 1], n_col)
        all_but_one(m, all_land, stat_send.at[m, 2], n_row * n_col)

    barrier = pltpu.get_barrier_semaphore()
    row_copy = pltpu.make_async_copy(row_hbm, row_moment, m_sem.at[0])
    col_copy = pltpu.make_async_copy(col_hbm, col_moment, m_sem.at[1])

    def greet_row(d, _):
        pl.semaphore_signal(
            barrier, inc=1, device_id=row_peer(d), device_id_type=MESH
        )
        return 0

    start_load(0)
    for axis in range(2):
        for to in (1, -1):
            pl.semaphore_signal(
                barrier, inc=1, device_id=neighbour(axis, to), device_id_type=MESH
            )
    lax.fori_loop(1, n_row, greet_row, 0)
    col_part[...] = jnp.zeros_like(col_part)
    row_copy.start()
    col_copy.start()
    load(0, 0).wait()
    prepare_relay(0, 0)
    pl.semaphore_wait(barrier, 4 + n_row - 1)
    send_relay(0, 0)
    load(0, 1).wait()
    prepare_relay(0, 1)
    send_relay(0, 1)
    for k in range(1, 1 + X_AHEAD):
        start_load(k)
    for color in range(2):
        prepare_direct(0, color)
        send_direct(0, color)
    row_copy.wait()
    col_copy.wait()

    def step(it, _):
        @pl.when(it > 0)
        def _():
            stage0(it)

            @pl.when(it + X_AHEAD < chunks)
            def _():
                start_load(it + X_AHEAD)

        for lag, work, end in (
            (3, stage2_direct, per_mat),
            (1, stage1, chunks),
            (2, stage2, chunks),
            (3, stage3, chunks),
            (4, stage4, per_mat),
        ):

            @pl.when((it >= lag) & (it < end + lag))
            def _():
                work(it - lag)

        @pl.when(it + 1 < chunks)
        def _():
            prepare(it + 1)

        for when, work in (
            (per_mat + 3, early_sums),
            (per_mat + 3, share_sums),
            (per_mat + 5, share_clip),
            (per_mat + 7, finish),
        ):

            @pl.when(it == when)
            def _():
                work(0)

        return 0

    lax.fori_loop(0, chunks, step, 0)

    def direct(first, count):
        def one(k, _):
            stage2_direct(k)
            return 0

        lax.fori_loop(first, first + count, one, 0)

    last = chunks - 1
    share = per_mat // 4
    stage1(last)
    direct(per_mat, share)
    stage2(last - 1)
    stage3(last - 2)
    direct(per_mat + share, share)
    stage2(last)
    direct(per_mat + 2 * share, share)
    stage3(last - 1)
    direct(per_mat + 3 * share, per_mat - 3 * share)
    stage3(last)

    def finish_chunk(k, _):
        stage4(k)
        return 0

    lax.fori_loop(per_mat, last, finish_chunk, 0)
    early_sums(mats - 1)
    stage4(last)
    share_sums(mats - 1)
    share_clip(mats - 1)
    finish(mats - 1)

    def drain(slot, _):
        for color in range(2):
            wait_bytes(stage.at[slot, color], send0.at[slot, color])
            wait_bytes(land1.at[0, color], send1.at[slot, color])
            wait_bytes(land2.at[0, color], send2.at[slot, color])
            wait_bytes(land2.at[0, color], send3.at[slot, color])
        return 0

    lax.fori_loop(0, S_SLOTS, drain, 0)

    def drain_direct(slot, _):
        for color in range(2):
            wait_bytes(land2.at[0, color], send5.at[slot, color])
        return 0

    lax.fori_loop(0, per_mat, drain_direct, 0)


def finish_kernel(
    scaled, factor, new_rows, new_cols, update_hbm, rows_hbm, cols_hbm, out, sems
):
    mats, rows, width = scaled.shape
    pieces = 4
    last = mats - 1
    size = rows // pieces
    copies = []

    def start(src, dst):
        copy = pltpu.make_async_copy(src, dst, sems.at[len(copies)])
        copy.start()
        copies.append(copy)

    for m in range(last):
        start(scaled.at[m], update_hbm.at[m])
    scale = jnp.broadcast_to(factor[last][:, :1], (TILE, width))
    for p in range(pieces):
        for t in range(p * size, (p + 1) * size, TILE):
            r = slice(t, t + TILE)
            out[r, :] = scaled[last, r, :] * scale
        here = pl.ds(p * size, size)
        start(out.at[here], update_hbm.at[last, here])
    start(new_rows, rows_hbm)
    start(new_cols, cols_hbm)
    for copy in copies:
        copy.wait()


def on_device(grad_terms, row_moment, col_moment):
    _, mats, rows, _ = grad_terms.shape
    width = col_moment.shape[1]
    n_row = lax.axis_size("row_0") * lax.axis_size("row_1")
    n_col = RING * RING
    chunks = mats * rows // (2 * CHUNK)
    f32 = jnp.float32
    vmem = pl.BlockSpec(memory_space=pltpu.VMEM)
    hbm = pl.BlockSpec(memory_space=pltpu.HBM)
    dma = pltpu.SemaphoreType.DMA
    shapes = (
        jax.ShapeDtypeStruct((mats, rows, width), f32),
        jax.ShapeDtypeStruct((mats, TILE, LANES), f32),
        jax.ShapeDtypeStruct((mats, rows), f32),
        jax.ShapeDtypeStruct((mats, width), f32),
    )
    scaled, factor, new_rows, new_cols = pl.pallas_call(
        kernel,
        out_shape=shapes,
        in_specs=[hbm, hbm, hbm],
        out_specs=(vmem, vmem, vmem, vmem),
        scratch_shapes=[
            pltpu.VMEM((X_SLOTS, 2, CHUNK, n_col * width), jnp.bfloat16),
            pltpu.VMEM((S_SLOTS, 2, 4, HALF, RING * width), f32),
            pltpu.VMEM((chunks, 2, 2, HALF, RING * width), f32),
            pltpu.VMEM((chunks, 2, 4, HALF, RING * width), f32),
            pltpu.VMEM((chunks, 2, 2, HALF, width), f32),
            pltpu.VMEM((chunks, 2, 4, HALF, width), f32),
            pltpu.VMEM((mats, rows), f32),
            pltpu.VMEM((mats, width), f32),
            pltpu.VMEM((mats, rows, LANES), f32),
            pltpu.VMEM((mats, TILE, width), f32),
            pltpu.VMEM((rows, LANES), f32),
            pltpu.VMEM((rows // LANES, LANES), f32),
            pltpu.VMEM((rows, LANES), f32),
            pltpu.VMEM((mats, n_col, rows // LANES, LANES), f32),
            pltpu.VMEM((mats, n_row, 1, width), f32),
            pltpu.VMEM((mats, n_row * n_col, 2, LANES), f32),
            dma((X_SLOTS, 2)),
            dma((2,)),
            dma((S_SLOTS, 2)),
            dma((S_SLOTS, 2)),
            dma((S_SLOTS, 2)),
            dma((S_SLOTS, 2)),
            dma((chunks // mats, 2)),
            dma((R_SLOTS, 2)),
            dma((R_SLOTS, 2)),
            dma((R_SLOTS, 2)),
            dma((chunks, 2)),
            dma((mats, 3)),
            dma((mats, 3)),
        ],
        compiler_params=pltpu.CompilerParams(
            collective_id=0,
            has_side_effects=True,
            vmem_limit_bytes=50 * 1024 * 1024,
        ),
    )(
        grad_terms,
        pltpu.with_memory_space_constraint(row_moment, pltpu.HBM),
        pltpu.with_memory_space_constraint(col_moment, pltpu.HBM),
    )
    return pl.pallas_call(
        finish_kernel,
        out_shape=(shapes[0], shapes[2], shapes[3]),
        in_specs=[vmem] * 4,
        out_specs=(hbm, hbm, hbm),
        scratch_shapes=[pltpu.VMEM((rows, width), f32), dma((8,))],
        compiler_params=pltpu.CompilerParams(vmem_limit_bytes=4 * 1024 * 1024),
    )(scaled, factor, new_rows, new_cols)


def solution(mesh):
    n_row = mesh.shape["row"]
    core = 2 if n_row > 1 else 1
    torus = Mesh(
        mesh.devices.reshape(n_row // core, core, RING, RING), ROW + COL
    )
    in_specs = (P(COL, None, ROW, None), P(None, ROW), P(None, COL))
    out_specs = (P(None, ROW, COL), P(None, ROW), P(None, COL))
    return jax.shard_map(
        on_device, mesh=torus, in_specs=in_specs, out_specs=out_specs, check_vma=False
    )
```

```python
import functools

import jax
import jax.numpy as jnp
from jax import lax
from jax.experimental import pallas as pl
from jax.experimental.pallas import tpu as pltpu
from jax.sharding import Mesh
from jax.sharding import PartitionSpec as P

MESH = pl.DeviceIdType.MESH
COL = ("col_0", "col_1")
ROW = ("row_0", "row_1")
RING = 4
LANES = 128
HALF = 16
CHUNK = 2 * HALF
X_SLOTS = 5
X_AHEAD = 2
S_SLOTS = 3
TILE = 8
R_SLOTS = 5

second_decay = 1.0 - 100.0 ** (-0.8)
tiny_square = 1e-30


def far_first(n_z, n_core):
    def hops(step, n):
        return min(step, n - step)

    steps = [
        (z, core, x, y)
        for z in range(n_z)
        for core in range(n_core)
        for x in range(RING)
        for y in range(RING)
    ]
    steps.sort(
        key=lambda s: -(hops(s[0], n_z) + hops(s[2], RING) + hops(s[3], RING))
    )
    return [s for s in steps if any(s)]


def wait_bytes(ref, sem):
    pltpu.make_async_copy(ref, ref, sem).wait()


def kernel(
    grad_hbm,
    row_hbm,
    col_hbm,
    update,
    factor,
    new_rows,
    new_cols,
    x_in,
    stage,
    land1,
    sum1,
    land2,
    sum2,
    row_moment,
    col_moment,
    row_part,
    col_part,
    weighted,
    weighted_row,
    row_scale,
    row_land,
    col_land,
    all_land,
    x_sem,
    m_sem,
    send0,
    send1,
    send2,
    send3,
    send5,
    recv1,
    recv2,
    recv3,
    recv4,
    greet,
    stat_send,
    stat_recv,
):
    mats, rows = row_moment.shape
    offsets = far_first(lax.axis_size("row_0"), lax.axis_size("row_1"))
    width = col_moment.shape[1]
    block = RING * width
    row_groups = rows // LANES
    n_row0, n_row1 = lax.axis_size("row_0"), lax.axis_size("row_1")
    n_row, n_col = n_row0 * n_row1, RING * RING
    total_rows = n_row * rows
    total_cols = n_col * width
    per_mat = rows // (2 * CHUNK)
    chunks = mats * per_mat

    here = (lax.axis_index("col_0"), lax.axis_index("col_1"))
    my_col = here[0] * RING + here[1]
    my_row = lax.axis_index("row_0") * n_row1 + lax.axis_index("row_1")

    def at(axis, step):
        return lax.rem(here[axis] + (step + RING), RING)

    me = my_row * n_col + my_col

    def neighbour(axis, step):
        return {COL[axis]: at(axis, step)}

    def col_peer(d):
        t = lax.rem(my_col + d, n_col)
        return {"col_0": t // RING, "col_1": lax.rem(t, RING)}

    def row_peer(d):
        t = lax.rem(my_row + d, n_row)
        return {"row_0": t // n_row1, "row_1": lax.rem(t, n_row1)}

    def send(src, dst, s_sem, r_sem, device):
        pltpu.make_async_remote_copy(
            src_ref=src,
            dst_ref=dst,
            send_sem=s_sem,
            recv_sem=r_sem,
            device_id=device,
            device_id_type=MESH,
        ).start()

    def load(k, color):
        slot = lax.rem(k, X_SLOTS)
        m = k // per_mat
        r = lax.rem(k, per_mat) * (2 * CHUNK) + color * CHUNK
        return pltpu.make_async_copy(
            grad_hbm.at[0, m, pl.ds(pl.multiple_of(r, CHUNK), CHUNK), :],
            x_in.at[slot, color],
            x_sem.at[slot, color],
        )

    def start_load(k):
        for color in range(2):
            load(k, color).start()

    def own(color, k, idx, seg):
        outer, inner = (idx, seg) if color == 0 else (seg, idx)
        c = pl.multiple_of(outer * block + inner * width, LANES)
        v = x_in[lax.rem(k, X_SLOTS), color, :, pl.ds(c, width)].astype(jnp.float32)
        return v[:HALF], v[HALF:]

    def cols(s):
        return slice(s * width, (s + 1) * width)

    def inner_cols(idx):
        return pl.ds(pl.multiple_of(idx * width, LANES), width)

    def free_stage(k, color):
        slot = lax.rem(k, S_SLOTS)

        @pl.when(k >= S_SLOTS)
        def _():
            wait_bytes(stage.at[slot, color], send0.at[slot, color])

    def prepare_relay(k, color):
        slot = lax.rem(k, S_SLOTS)
        for s in range(RING):
            top, low = own(color, k, at(color, 2), s)
            stage[slot, color, 0, :, cols(s)] = top
            stage[slot, color, 1, :, cols(s)] = low

    def prepare_direct(k, color):
        slot = lax.rem(k, S_SLOTS)
        for s in range(RING):
            _, low = own(color, k, at(color, 1), s)
            stage[slot, color, 2, :, cols(s)] = low
            top, _ = own(color, k, at(color, -1), s)
            stage[slot, color, 3, :, cols(s)] = top

    def prepare(k):
        for color in range(2):
            load(k, color).wait()
            free_stage(k, color)
            prepare_relay(k, color)
            prepare_direct(k, color)

    def send_relay(k, color):
        slot = lax.rem(k, S_SLOTS)
        for which, step in ((0, 1), (1, -1)):
            send(
                stage.at[slot, color, which],
                land1.at[k, color, which],
                send0.at[slot, color],
                recv1.at[lax.rem(k, R_SLOTS), color],
                neighbour(color, step),
            )

    def send_direct(k, color):
        slot = lax.rem(k, S_SLOTS)
        for which, step in ((2, 1), (3, -1)):
            send(
                stage.at[slot, color, which],
                sum1.at[k, color, which],
                send0.at[slot, color],
                recv2.at[lax.rem(k, R_SLOTS), color],
                neighbour(color, step),
            )

    def stage0(k):
        for color in range(2):
            send_relay(k, color)
        for color in range(2):
            send_direct(k, color)

    def stage1(k):
        for color in range(2):
            axis = color
            wait_bytes(land1.at[k, color], recv1.at[lax.rem(k, R_SLOTS), color])

            for s in range(RING):
                top, _ = own(color, k, at(axis, 1), s)
                land1[k, color, 0, :, cols(s)] = land1[k, color, 0, :, cols(s)] + top
                _, low = own(color, k, at(axis, -1), s)
                land1[k, color, 1, :, cols(s)] = land1[k, color, 1, :, cols(s)] + low
            for which, step in ((0, 1), (1, -1)):
                send(
                    land1.at[k, color, which],
                    sum1.at[k, color, which],
                    send1.at[color],
                    recv2.at[lax.rem(k, R_SLOTS), color],
                    neighbour(axis, step),
                )

    def stage2(k):
        for color in range(2):
            axis = color
            wait_bytes(sum1.at[k, color], recv2.at[lax.rem(k, R_SLOTS), color])

            for s in range(RING):
                top, low = own(color, k, at(axis, 0), s)
                sum1[k, color, 0, :, cols(s)] = (
                    sum1[k, color, 0, :, cols(s)]
                    + sum1[k, color, 3, :, cols(s)]
                    + top
                )
                sum1[k, color, 1, :, cols(s)] = (
                    sum1[k, color, 1, :, cols(s)]
                    + sum1[k, color, 2, :, cols(s)]
                    + low
                )
            axis = 1 - color
            for which, step in ((0, 1), (1, -1)):
                send(
                    sum1.at[k, color, which, :, inner_cols(at(axis, 2))],
                    land2.at[k, color, which],
                    send2.at[color],
                    recv3.at[lax.rem(k, R_SLOTS), color],
                    neighbour(axis, step),
                )

    def stage2_direct(k):
        for color in range(2):
            axis = 1 - color
            for half, which, step in ((1, 2, 1), (0, 3, -1)):
                send(
                    sum1.at[k, color, half, :, inner_cols(at(axis, step))],
                    sum2.at[k, color, which],
                    send5.at[color],
                    recv4.at[k],
                    neighbour(axis, step),
                )

    def stage3(k):
        for color in range(2):
            axis = 1 - color
            wait_bytes(land2.at[k, color], recv3.at[lax.rem(k, R_SLOTS), color])

            for which, step in ((0, 1), (1, -1)):
                land2[k, color, which] = (
                    land2[k, color, which]
                    + sum1[k, color, which, :, inner_cols(at(axis, step))]
                )
                send(
                    land2.at[k, color, which],
                    sum2.at[k, color, which],
                    send3.at[color],
                    recv4.at[k],
                    neighbour(axis, step),
                )

    def lane_tiles(v):
        out = v[:, :LANES]
        for c in range(1, width // LANES):
            out = out + v[:, c * LANES : (c + 1) * LANES]
        return out

    def stage4(k):
        m = k // per_mat
        r = lax.rem(k, per_mat) * (2 * CHUNK)
        squares_sum = col_part[m]
        wait_bytes(sum2.at[k], recv4.at[k])
        for color in range(2):
            axis = 1 - color
            for half, other in ((0, 3), (1, 2)):
                g = (
                    sum2[k, color, half]
                    + sum2[k, color, other]
                    + sum1[k, color, half, :, inner_cols(at(axis, 0))]
                )
                here_rows = pl.ds(
                    pl.multiple_of(r + color * CHUNK + half * HALF, HALF), HALF
                )
                update[m, here_rows, :] = g
                squares = g * g + tiny_square
                row_part[m, here_rows, :] = lane_tiles(squares)
                for t in range(HALF // TILE):
                    squares_sum = squares_sum + squares[t * TILE : (t + 1) * TILE]
        col_part[m] = squares_sum

    def pick(ref, m, lanes):
        return jnp.where(m == 0, ref[0:1, lanes], ref[1:2, lanes])

    def put(ref, m, lanes, value):
        for i in range(mats):

            @pl.when(m == i)
            def _():
                ref[i : i + 1, lanes] = value

    def lane_major(part):
        return jnp.sum(part.T, axis=0, keepdims=True)

    def group(b):
        return slice(b * LANES, (b + 1) * LANES)

    def early_sums(m):
        for b in range(row_groups - 1):
            row_land[m, my_col, b : b + 1, :] = lane_major(row_part[m, group(b), :])

    def peer(step):
        z, core, x, y = step
        there = {}
        if z or core:
            there["row_0"] = lax.rem(lax.axis_index("row_0") + z, n_row0)
            there["row_1"] = lax.rem(lax.axis_index("row_1") + core, n_row1)
        if x or y:
            there["col_0"] = at(0, x)
            there["col_1"] = at(1, y)
        return there

    def share_sums(m):
        col_land[m, my_row] = jnp.sum(col_part[m], axis=0, keepdims=True)
        mine = col_land.at[m, my_row]
        for step in offsets:
            if not any(step[2:]):
                send(mine, mine, stat_send.at[m, 0], stat_recv.at[m, 0], peer(step))
        b = row_groups - 1
        row_land[m, my_col, b : b + 1, :] = lane_major(row_part[m, group(b), :])
        rows_mine = row_land.at[m, my_col]
        for step in offsets:
            if not any(step[:2]):
                send(
                    rows_mine,
                    rows_mine,
                    stat_send.at[m, 1],
                    stat_recv.at[m, 1],
                    peer(step),
                )

    def all_but_one(m, buf, sem, n):
        if n > 1:
            wait_bytes(buf.at[m, pl.ds(0, n - 1)], sem)

    def share_clip(m):
        all_but_one(m, col_land, stat_recv.at[m, 0], n_row)
        full = col_land[m, 0]
        for s in range(1, n_row):
            full = full + col_land[m, s]
        col = (
            second_decay * pick(col_moment, m, slice(None))
            + (1.0 - second_decay) * full / total_rows
        )
        inverse = jnp.broadcast_to(1.0 / col, (TILE, width))

        def weigh(t, _):
            r = pl.ds(pl.multiple_of(t * TILE, TILE), TILE)
            v = update[m, r, :]
            weighted[r, :] = lane_tiles(v * v * inverse)
            return 0

        lax.fori_loop(0, rows // TILE, weigh, 0, unroll=8)
        for b in range(row_groups):
            weighted_row[b : b + 1, :] = lane_major(weighted[group(b), :])

        all_but_one(m, row_land, stat_recv.at[m, 1], n_col)
        full = row_land[m, 0]
        for s in range(1, n_col):
            full = full + row_land[m, s]
        moments, clip, level = [], None, None
        for b in range(row_groups):
            moment = (
                second_decay * pick(row_moment, m, group(b))
                + (1.0 - second_decay) * full[b : b + 1] / total_cols
            )
            part = weighted_row[b : b + 1, :] / moment
            clip = part if clip is None else clip + part
            level = moment if level is None else level + moment
            moments.append(moment)
        all_land[m, me, 0:1, :] = clip
        all_land[m, me, 1:2, :] = level
        mine = all_land.at[m, me]
        for step in offsets:
            send(mine, mine, stat_send.at[m, 2], stat_recv.at[m, 2], peer(step))
        put(new_cols, m, slice(None), col)
        for b in range(row_groups):
            put(new_rows, m, group(b), moments[b])
            row_scale[group(b), :] = jnp.broadcast_to(
                lax.rsqrt(moments[b]), (LANES, LANES)
            ).T
        col_scale = jnp.broadcast_to(lax.rsqrt(col), (TILE, width))

        def rescale(t, _):
            r = pl.ds(pl.multiple_of(t * TILE, TILE), TILE)
            scale = row_scale[r, :]
            for c in range(width // LANES):
                lanes = group(c)
                update[m, r, lanes] = update[m, r, lanes] * col_scale[:, lanes] * scale
            return 0

        lax.fori_loop(0, rows // TILE, rescale, 0, unroll=8)

    def finish(m):
        all_but_one(m, all_land, stat_recv.at[m, 2], n_row * n_col)
        parts = [all_land[m, s] for s in range(4)]
        for s in range(4, n_row * n_col):
            parts[s % 4] = parts[s % 4] + all_land[m, s]
        total = (parts[0] + parts[1]) + (parts[2] + parts[3])
        level = jnp.sum(total[1:2], axis=1, keepdims=True) / (n_col * total_rows)
        clip = jnp.sum(total[0:1], axis=1, keepdims=True)
        clip_scale = jnp.maximum(
            1.0, jnp.sqrt(clip * level / (total_rows * total_cols))
        )
        scale = jnp.broadcast_to(jnp.sqrt(level) / clip_scale, (TILE, LANES))
        factor[m] = scale

        @pl.when(m < mats - 1)
        def _():
            wide = jnp.broadcast_to(scale[:, :1], (TILE, width))

            def one(t, _):
                r = pl.ds(pl.multiple_of(t * TILE, TILE), TILE)
                update[m, r, :] = update[m, r, :] * wide
                return 0

            lax.fori_loop(0, rows // TILE, one, 0, unroll=4)

        all_but_one(m, col_land, stat_send.at[m, 0], n_row)
        all_but_one(m, row_land, stat_send.at[m, 1], n_col)
        all_but_one(m, all_land, stat_send.at[m, 2], n_row * n_col)

    barrier = pltpu.get_barrier_semaphore()
    row_copy = pltpu.make_async_copy(row_hbm, row_moment, m_sem.at[0])
    col_copy = pltpu.make_async_copy(col_hbm, col_moment, m_sem.at[1])

    near = [t for t in offsets if not any(t[2:])]
    near = [t for t in near if t in ((1, 0, 0, 0), (n_row0 - 1, 0, 0, 0), (0, 1, 0, 0))]

    def greet_near(sem):
        for step in near:
            pl.semaphore_signal(
                sem, inc=1, device_id=peer(step), device_id_type=MESH
            )

    start_load(0)
    for axis in range(2):
        for to in (1, -1):
            pl.semaphore_signal(
                barrier, inc=1, device_id=neighbour(axis, to), device_id_type=MESH
            )
    greet_near(barrier)
    col_part[...] = jnp.zeros_like(col_part)
    row_copy.start()
    col_copy.start()
    load(0, 0).wait()
    prepare_relay(0, 0)
    pl.semaphore_wait(barrier, 4 + len(near))
    send_relay(0, 0)
    load(0, 1).wait()
    prepare_relay(0, 1)
    send_relay(0, 1)
    for k in range(1, 1 + X_AHEAD):
        start_load(k)
    for color in range(2):
        prepare_direct(0, color)
        send_direct(0, color)
    greet_near(greet.at[0])
    row_copy.wait()
    col_copy.wait()

    def step(it, _):
        @pl.when(it > 0)
        def _():
            stage0(it)

            @pl.when(it + X_AHEAD < chunks)
            def _():
                start_load(it + X_AHEAD)

        for lag, work, end in (
            (3, stage2_direct, per_mat),
            (1, stage1, chunks),
            (2, stage2, chunks),
            (3, stage3, chunks),
            (4, stage4, per_mat),
        ):

            @pl.when((it >= lag) & (it < end + lag))
            def _():
                work(it - lag)

        @pl.when(it + 1 < chunks)
        def _():
            prepare(it + 1)

        @pl.when(it == 1)
        def _():
            pl.semaphore_wait(greet.at[0], len(near))
            greet_near(greet.at[1])

        @pl.when(it == 2)
        def _():
            pl.semaphore_wait(greet.at[1], len(near))

        for when, work in (
            (per_mat + 3, early_sums),
            (per_mat + 3, share_sums),
            (per_mat + 5, share_clip),
            (per_mat + 7, finish),
        ):

            @pl.when(it == when)
            def _():
                work(0)

        return 0

    lax.fori_loop(0, chunks, step, 0)

    def direct(first, count):
        def one(k, _):
            stage2_direct(k)
            return 0

        lax.fori_loop(first, first + count, one, 0)

    last = chunks - 1
    share = per_mat // 4
    stage1(last)
    direct(per_mat, share)
    stage2(last - 1)
    stage3(last - 2)
    direct(per_mat + share, share)
    stage2(last)
    direct(per_mat + 2 * share, share)
    stage3(last - 1)
    direct(per_mat + 3 * share, per_mat - 3 * share)
    stage3(last)

    def finish_chunk(k, _):
        stage4(k)
        return 0

    lax.fori_loop(per_mat, last, finish_chunk, 0)
    early_sums(mats - 1)
    stage4(last)
    share_sums(mats - 1)
    share_clip(mats - 1)
    finish(mats - 1)

    for color in range(2):
        for slot in range(S_SLOTS):
            wait_bytes(stage.at[slot, color], send0.at[slot, color])
        wait_bytes(land1.at[:, color], send1.at[color])
        wait_bytes(land2.at[:, color], send2.at[color])
        wait_bytes(land2.at[:, color], send3.at[color])
        wait_bytes(land2.at[:, color], send5.at[color])


def finish_kernel(
    scaled, factor, new_rows, new_cols, update_hbm, rows_hbm, cols_hbm, out, sems
):
    mats, rows, width = scaled.shape
    pieces = 4
    last = mats - 1
    size = rows // pieces
    copies = []

    def start(src, dst):
        copy = pltpu.make_async_copy(src, dst, sems.at[len(copies)])
        copy.start()
        copies.append(copy)

    for m in range(last):
        start(scaled.at[m], update_hbm.at[m])
    scale = jnp.broadcast_to(factor[last][:, :1], (TILE, width))
    for p in range(pieces):
        for t in range(p * size, (p + 1) * size, TILE):
            r = slice(t, t + TILE)
            out[r, :] = scaled[last, r, :] * scale
        here = pl.ds(p * size, size)
        start(out.at[here], update_hbm.at[last, here])
    start(new_rows, rows_hbm)
    start(new_cols, cols_hbm)
    for copy in copies:
        copy.wait()


def on_device(grad_terms, row_moment, col_moment):
    _, mats, rows, _ = grad_terms.shape
    width = col_moment.shape[1]
    n_row = lax.axis_size("row_0") * lax.axis_size("row_1")
    n_col = RING * RING
    chunks = mats * rows // (2 * CHUNK)
    f32 = jnp.float32
    vmem = pl.BlockSpec(memory_space=pltpu.VMEM)
    hbm = pl.BlockSpec(memory_space=pltpu.HBM)
    dma = pltpu.SemaphoreType.DMA
    shapes = (
        jax.ShapeDtypeStruct((mats, rows, width), f32),
        jax.ShapeDtypeStruct((mats, TILE, LANES), f32),
        jax.ShapeDtypeStruct((mats, rows), f32),
        jax.ShapeDtypeStruct((mats, width), f32),
    )
    scaled, factor, new_rows, new_cols = pl.pallas_call(
        kernel,
        out_shape=shapes,
        in_specs=[hbm, hbm, hbm],
        out_specs=(vmem, vmem, vmem, vmem),
        scratch_shapes=[
            pltpu.VMEM((X_SLOTS, 2, CHUNK, n_col * width), jnp.bfloat16),
            pltpu.VMEM((S_SLOTS, 2, 4, HALF, RING * width), f32),
            pltpu.VMEM((chunks, 2, 2, HALF, RING * width), f32),
            pltpu.VMEM((chunks, 2, 4, HALF, RING * width), f32),
            pltpu.VMEM((chunks, 2, 2, HALF, width), f32),
            pltpu.VMEM((chunks, 2, 4, HALF, width), f32),
            pltpu.VMEM((mats, rows), f32),
            pltpu.VMEM((mats, width), f32),
            pltpu.VMEM((mats, rows, LANES), f32),
            pltpu.VMEM((mats, TILE, width), f32),
            pltpu.VMEM((rows, LANES), f32),
            pltpu.VMEM((rows // LANES, LANES), f32),
            pltpu.VMEM((rows, LANES), f32),
            pltpu.VMEM((mats, n_col, rows // LANES, LANES), f32),
            pltpu.VMEM((mats, n_row, 1, width), f32),
            pltpu.VMEM((mats, n_row * n_col, 2, LANES), f32),
            dma((X_SLOTS, 2)),
            dma((2,)),
            dma((S_SLOTS, 2)),
            dma((2,)),
            dma((2,)),
            dma((2,)),
            dma((2,)),
            dma((R_SLOTS, 2)),
            dma((R_SLOTS, 2)),
            dma((R_SLOTS, 2)),
            dma((chunks,)),
            pltpu.SemaphoreType.REGULAR((2,)),
            dma((mats, 3)),
            dma((mats, 3)),
        ],
        compiler_params=pltpu.CompilerParams(
            collective_id=0,
            has_side_effects=True,
            vmem_limit_bytes=50 * 1024 * 1024,
        ),
    )(
        grad_terms,
        pltpu.with_memory_space_constraint(row_moment, pltpu.HBM),
        pltpu.with_memory_space_constraint(col_moment, pltpu.HBM),
    )
    return pl.pallas_call(
        finish_kernel,
        out_shape=(shapes[0], shapes[2], shapes[3]),
        in_specs=[vmem] * 4,
        out_specs=(hbm, hbm, hbm),
        scratch_shapes=[pltpu.VMEM((rows, width), f32), dma((8,))],
        compiler_params=pltpu.CompilerParams(vmem_limit_bytes=4 * 1024 * 1024),
    )(scaled, factor, new_rows, new_cols)


def solution(mesh):
    n_row = mesh.shape["row"]
    core = 2 if n_row > 1 else 1
    torus = Mesh(
        mesh.devices.reshape(n_row // core, core, RING, RING), ROW + COL
    )
    in_specs = (P(COL, None, ROW, None), P(None, ROW), P(None, COL))
    out_specs = (P(None, ROW, COL), P(None, ROW), P(None, COL))
    return jax.shard_map(
        on_device, mesh=torus, in_specs=in_specs, out_specs=out_specs, check_vma=False
    )
```

```python
import functools

import jax
import jax.numpy as jnp
from jax import lax
from jax.experimental import pallas as pl
from jax.experimental.pallas import tpu as pltpu
from jax.sharding import Mesh
from jax.sharding import PartitionSpec as P

MESH = pl.DeviceIdType.MESH
COL = ("col_0", "col_1")
ROW = ("row_0", "row_1")
RING = 4
LANES = 128
HALF = 16
CHUNK = 2 * HALF
X_SLOTS = 5
X_AHEAD = 2
S_SLOTS = 3
TILE = 8
R_SLOTS = 5

second_decay = 1.0 - 100.0 ** (-0.8)
tiny_square = 1e-30


def far_first(n_z, n_core):
    def hops(step, n):
        return min(step, n - step)

    steps = [
        (z, core, x, y)
        for z in range(n_z)
        for core in range(n_core)
        for x in range(RING)
        for y in range(RING)
    ]
    steps.sort(
        key=lambda s: -(hops(s[0], n_z) + hops(s[2], RING) + hops(s[3], RING))
    )
    return [s for s in steps if any(s)]


def wait_bytes(ref, sem):
    pltpu.make_async_copy(ref, ref, sem).wait()


def kernel(
    grad_hbm,
    row_hbm,
    col_hbm,
    update,
    factor,
    new_rows,
    new_cols,
    x_in,
    stage,
    land1,
    sum1,
    land2,
    sum2,
    row_moment,
    col_moment,
    row_part,
    col_part,
    weighted,
    weighted_row,
    row_scale,
    row_land,
    col_land,
    all_land,
    late_land,
    late_all,
    x_sem,
    m_sem,
    send0,
    send1,
    send2,
    send3,
    send5,
    recv1,
    recv2,
    recv3,
    recv4,
    greet,
    stat_send,
    stat_recv,
):
    mats, rows = row_moment.shape
    offsets = far_first(lax.axis_size("row_0"), lax.axis_size("row_1"))
    width = col_moment.shape[1]
    block = RING * width
    row_groups = rows // LANES
    n_row0, n_row1 = lax.axis_size("row_0"), lax.axis_size("row_1")
    n_row, n_col = n_row0 * n_row1, RING * RING
    total_rows = n_row * rows
    total_cols = n_col * width
    per_mat = rows // (2 * CHUNK)
    chunks = mats * per_mat

    here = (lax.axis_index("col_0"), lax.axis_index("col_1"))
    my_col = here[0] * RING + here[1]
    my_row = lax.axis_index("row_0") * n_row1 + lax.axis_index("row_1")

    def at(axis, step):
        return lax.rem(here[axis] + (step + RING), RING)

    me = my_row * n_col + my_col

    def neighbour(axis, step):
        return {COL[axis]: at(axis, step)}

    def col_peer(d):
        t = lax.rem(my_col + d, n_col)
        return {"col_0": t // RING, "col_1": lax.rem(t, RING)}

    def row_peer(d):
        t = lax.rem(my_row + d, n_row)
        return {"row_0": t // n_row1, "row_1": lax.rem(t, n_row1)}

    def send(src, dst, s_sem, r_sem, device):
        pltpu.make_async_remote_copy(
            src_ref=src,
            dst_ref=dst,
            send_sem=s_sem,
            recv_sem=r_sem,
            device_id=device,
            device_id_type=MESH,
        ).start()

    def load(k, color):
        slot = lax.rem(k, X_SLOTS)
        m = k // per_mat
        r = lax.rem(k, per_mat) * (2 * CHUNK) + color * CHUNK
        return pltpu.make_async_copy(
            grad_hbm.at[0, m, pl.ds(pl.multiple_of(r, CHUNK), CHUNK), :],
            x_in.at[slot, color],
            x_sem.at[slot, color],
        )

    def start_load(k):
        for color in range(2):
            load(k, color).start()

    def own(color, k, idx, seg):
        outer, inner = (idx, seg) if color == 0 else (seg, idx)
        c = pl.multiple_of(outer * block + inner * width, LANES)
        v = x_in[lax.rem(k, X_SLOTS), color, :, pl.ds(c, width)].astype(jnp.float32)
        return v[:HALF], v[HALF:]

    def cols(s):
        return slice(s * width, (s + 1) * width)

    def inner_cols(idx):
        return pl.ds(pl.multiple_of(idx * width, LANES), width)

    def free_stage(k, color):
        slot = lax.rem(k, S_SLOTS)

        @pl.when(k >= S_SLOTS)
        def _():
            wait_bytes(stage.at[slot, color], send0.at[slot, color])

    def prepare_relay(k, color):
        slot = lax.rem(k, S_SLOTS)
        for s in range(RING):
            top, low = own(color, k, at(color, 2), s)
            stage[slot, color, 0, :, cols(s)] = top
            stage[slot, color, 1, :, cols(s)] = low

    def prepare_direct(k, color):
        slot = lax.rem(k, S_SLOTS)
        for s in range(RING):
            _, low = own(color, k, at(color, 1), s)
            stage[slot, color, 2, :, cols(s)] = low
            top, _ = own(color, k, at(color, -1), s)
            stage[slot, color, 3, :, cols(s)] = top

    def prepare(k):
        for color in range(2):
            load(k, color).wait()
            free_stage(k, color)
            prepare_relay(k, color)
            prepare_direct(k, color)

    def send_relay(k, color):
        slot = lax.rem(k, S_SLOTS)
        for which, step in ((0, 1), (1, -1)):
            send(
                stage.at[slot, color, which],
                land1.at[k, color, which],
                send0.at[slot, color],
                recv1.at[lax.rem(k, R_SLOTS), color],
                neighbour(color, step),
            )

    def send_direct(k, color):
        slot = lax.rem(k, S_SLOTS)
        for which, step in ((2, 1), (3, -1)):
            send(
                stage.at[slot, color, which],
                sum1.at[k, color, which],
                send0.at[slot, color],
                recv2.at[lax.rem(k, R_SLOTS), color],
                neighbour(color, step),
            )

    def stage0(k):
        for color in range(2):
            send_relay(k, color)
        for color in range(2):
            send_direct(k, color)

    def stage1(k):
        for color in range(2):
            axis = color
            wait_bytes(land1.at[k, color], recv1.at[lax.rem(k, R_SLOTS), color])

            for s in range(RING):
                top, _ = own(color, k, at(axis, 1), s)
                land1[k, color, 0, :, cols(s)] = land1[k, color, 0, :, cols(s)] + top
                _, low = own(color, k, at(axis, -1), s)
                land1[k, color, 1, :, cols(s)] = land1[k, color, 1, :, cols(s)] + low
            for which, step in ((0, 1), (1, -1)):
                send(
                    land1.at[k, color, which],
                    sum1.at[k, color, which],
                    send1.at[color],
                    recv2.at[lax.rem(k, R_SLOTS), color],
                    neighbour(axis, step),
                )

    def stage2(k):
        for color in range(2):
            axis = color
            wait_bytes(sum1.at[k, color], recv2.at[lax.rem(k, R_SLOTS), color])

            for s in range(RING):
                top, low = own(color, k, at(axis, 0), s)
                sum1[k, color, 0, :, cols(s)] = (
                    sum1[k, color, 0, :, cols(s)]
                    + sum1[k, color, 3, :, cols(s)]
                    + top
                )
                sum1[k, color, 1, :, cols(s)] = (
                    sum1[k, color, 1, :, cols(s)]
                    + sum1[k, color, 2, :, cols(s)]
                    + low
                )
            axis = 1 - color
            for which, step in ((0, 1), (1, -1)):
                send(
                    sum1.at[k, color, which, :, inner_cols(at(axis, 2))],
                    land2.at[k, color, which],
                    send2.at[color],
                    recv3.at[lax.rem(k, R_SLOTS), color],
                    neighbour(axis, step),
                )

    def stage2_direct(k):
        for color in range(2):
            axis = 1 - color
            for half, which, step in ((1, 2, 1), (0, 3, -1)):
                send(
                    sum1.at[k, color, half, :, inner_cols(at(axis, step))],
                    sum2.at[k, color, which],
                    send5.at[color],
                    recv4.at[k],
                    neighbour(axis, step),
                )

    def stage3(k):
        for color in range(2):
            axis = 1 - color
            wait_bytes(land2.at[k, color], recv3.at[lax.rem(k, R_SLOTS), color])

            for which, step in ((0, 1), (1, -1)):
                land2[k, color, which] = (
                    land2[k, color, which]
                    + sum1[k, color, which, :, inner_cols(at(axis, step))]
                )
                send(
                    land2.at[k, color, which],
                    sum2.at[k, color, which],
                    send3.at[color],
                    recv4.at[k],
                    neighbour(axis, step),
                )

    def lane_tiles(v):
        out = v[:, :LANES]
        for c in range(1, width // LANES):
            out = out + v[:, c * LANES : (c + 1) * LANES]
        return out

    def stage4(k):
        m = k // per_mat
        r = lax.rem(k, per_mat) * (2 * CHUNK)
        squares_sum = col_part[m]
        wait_bytes(sum2.at[k], recv4.at[k])
        for color in range(2):
            axis = 1 - color
            for half, other in ((0, 3), (1, 2)):
                g = (
                    sum2[k, color, half]
                    + sum2[k, color, other]
                    + sum1[k, color, half, :, inner_cols(at(axis, 0))]
                )
                here_rows = pl.ds(
                    pl.multiple_of(r + color * CHUNK + half * HALF, HALF), HALF
                )
                update[m, here_rows, :] = g
                squares = g * g + tiny_square
                row_part[m, here_rows, :] = lane_tiles(squares)
                for t in range(HALF // TILE):
                    squares_sum = squares_sum + squares[t * TILE : (t + 1) * TILE]
        col_part[m] = squares_sum

    def pick(ref, m, lanes):
        return jnp.where(m == 0, ref[0:1, lanes], ref[1:2, lanes])

    def put(ref, m, lanes, value):
        for i in range(mats):

            @pl.when(m == i)
            def _():
                ref[i : i + 1, lanes] = value

    lane = lax.broadcasted_iota(jnp.int32, (1, LANES), 1)
    is_early = lane < LANES - 2 * CHUNK
    assert 2 * CHUNK == LANES // 2

    def lane_major(part):
        return jnp.sum(part.T, axis=0, keepdims=True)

    def group(b):
        return slice(b * LANES, (b + 1) * LANES)

    def peer(step):
        z, core, x, y = step
        there = {}
        if z or core:
            there["row_0"] = lax.rem(lax.axis_index("row_0") + z, n_row0)
            there["row_1"] = lax.rem(lax.axis_index("row_1") + core, n_row1)
        if x or y:
            there["col_0"] = at(0, x)
            there["col_1"] = at(1, y)
        return there

    def to_cols(m, buf, which):
        mine = buf.at[m, my_col]
        for step in offsets:
            if not any(step[:2]):
                send(
                    mine, mine, stat_send.at[m, which], stat_recv.at[m, which], peer(step)
                )

    def share_early(m):
        for b in range(row_groups):
            row_land[m, my_col, b : b + 1, :] = lane_major(row_part[m, group(b), :])
        to_cols(m, row_land, 1)

    def share_sums(m):
        col_land[m, my_row] = jnp.sum(col_part[m], axis=0, keepdims=True)
        mine = col_land.at[m, my_row]
        for step in offsets:
            if not any(step[2:]):
                send(mine, mine, stat_send.at[m, 0], stat_recv.at[m, 0], peer(step))
        late_land[m, my_col] = lane_major(row_part[m, group(row_groups - 1), :])
        to_cols(m, late_land, 3)

    def all_but_one(m, buf, sem, n):
        if n > 1:
            wait_bytes(buf.at[m, pl.ds(0, n - 1)], sem)

    def share_clip(m):
        all_but_one(m, col_land, stat_recv.at[m, 0], n_row)
        full = col_land[m, 0]
        for s in range(1, n_row):
            full = full + col_land[m, s]
        col = (
            second_decay * pick(col_moment, m, slice(None))
            + (1.0 - second_decay) * full / total_rows
        )
        inverse = jnp.broadcast_to(1.0 / col, (TILE, width))

        def weigh(t, _):
            r = pl.ds(pl.multiple_of(t * TILE, TILE), TILE)
            v = update[m, r, :]
            weighted[r, :] = lane_tiles(v * v * inverse)
            return 0

        lax.fori_loop(0, rows // TILE, weigh, 0, unroll=8)
        for b in range(row_groups):
            weighted_row[b : b + 1, :] = lane_major(weighted[group(b), :])

        all_but_one(m, row_land, stat_recv.at[m, 1], n_col)
        full = row_land[m, 0]
        for s in range(1, n_col):
            full = full + row_land[m, s]
        moments, clip, level = [], None, None
        for b in range(row_groups):
            moment = (
                second_decay * pick(row_moment, m, group(b))
                + (1.0 - second_decay) * full[b : b + 1] / total_cols
            )
            moments.append(moment)
            part = weighted_row[b : b + 1, :] / moment
            if b == row_groups - 1:
                part = jnp.where(is_early, part, 0.0)
                moment = jnp.where(is_early, moment, 0.0)
            clip = part if clip is None else clip + part
            level = moment if level is None else level + moment
        clip = clip + pltpu.roll(clip, LANES // 2, 1)
        level = level + pltpu.roll(level, LANES // 2, 1)
        late = (
            second_decay * pick(row_moment, m, group(row_groups - 1)) / n_col
            + (1.0 - second_decay) * late_land[m, my_col] / total_cols
        )
        late_weight = pltpu.roll(
            weighted_row[row_groups - 1 : row_groups, :], LANES // 2, 1
        )
        all_land[m, me, 0:1, :] = jnp.where(is_early, clip, level)
        all_land[m, me, 1:2, :] = jnp.where(is_early, late_weight, late)
        mine = all_land.at[m, me]
        for step in offsets:
            send(mine, mine, stat_send.at[m, 2], stat_recv.at[m, 2], peer(step))
        put(new_cols, m, slice(None), col)
        col_scale = jnp.broadcast_to(lax.rsqrt(col), (TILE, width))

        def rescale(t, _):
            r = pl.ds(pl.multiple_of(t * TILE, TILE), TILE)
            scale = row_scale[r, :]
            for c in range(width // LANES):
                lanes = group(c)
                update[m, r, lanes] = update[m, r, lanes] * col_scale[:, lanes] * scale
            return 0

        for b in range(row_groups - 1):
            put(new_rows, m, group(b), moments[b])
            row_scale[group(b), :] = jnp.broadcast_to(
                lax.rsqrt(moments[b]), (LANES, LANES)
            ).T
        tiles = (row_groups - 1) * LANES // TILE
        lax.fori_loop(0, tiles, rescale, 0, unroll=8)

        all_but_one(m, late_land, stat_recv.at[m, 3], n_col)
        full = late_land[m, 0]
        for s in range(1, n_col):
            full = full + late_land[m, s]
        b = row_groups - 1
        moment = (
            second_decay * pick(row_moment, m, group(b))
            + (1.0 - second_decay) * full / total_cols
        )
        moment = jnp.where(is_early, moments[b], moment)
        put(new_rows, m, group(b), moment)
        row_scale[group(b), :] = jnp.broadcast_to(lax.rsqrt(moment), (LANES, LANES)).T
        lax.fori_loop(tiles, rows // TILE, rescale, 0, unroll=8)

    def finish(m):
        all_but_one(m, all_land, stat_recv.at[m, 2], n_row * n_col)
        total = None
        for r in range(n_row):
            parts = [all_land[m, r * n_col + c] for c in range(4)]
            for c in range(4, n_col):
                parts[c % 4] = parts[c % 4] + all_land[m, r * n_col + c]
            one_row = (parts[0] + parts[1]) + (parts[2] + parts[3])
            total = one_row if total is None else total + one_row
            late_all[r : r + 1, :] = one_row[1:2]
        late = late_all[...]
        ratio = late / pltpu.roll(late, LANES // 2, 1)
        clip = jnp.where(is_early, total[0:1], 0.0) + jnp.sum(
            jnp.where(is_early, ratio, 0.0), axis=0, keepdims=True
        )
        level = jnp.where(is_early, 0.0, total[0:1] / n_col + total[1:2])
        clip = jnp.sum(clip, axis=1, keepdims=True)
        level = jnp.sum(level, axis=1, keepdims=True) / total_rows
        clip_scale = jnp.maximum(
            1.0, jnp.sqrt(clip * level / (total_rows * total_cols))
        )
        scale = jnp.broadcast_to(jnp.sqrt(level) / clip_scale, (TILE, LANES))
        factor[m] = scale

        @pl.when(m < mats - 1)
        def _():
            wide = jnp.broadcast_to(scale[:, :1], (TILE, width))

            def one(t, _):
                r = pl.ds(pl.multiple_of(t * TILE, TILE), TILE)
                update[m, r, :] = update[m, r, :] * wide
                return 0

            lax.fori_loop(0, rows // TILE, one, 0, unroll=4)

        all_but_one(m, col_land, stat_send.at[m, 0], n_row)
        all_but_one(m, row_land, stat_send.at[m, 1], n_col)
        all_but_one(m, all_land, stat_send.at[m, 2], n_row * n_col)
        all_but_one(m, late_land, stat_send.at[m, 3], n_col)

    barrier = pltpu.get_barrier_semaphore()
    row_copy = pltpu.make_async_copy(row_hbm, row_moment, m_sem.at[0])
    col_copy = pltpu.make_async_copy(col_hbm, col_moment, m_sem.at[1])

    near = [t for t in offsets if not any(t[2:])]
    near = [t for t in near if t in ((1, 0, 0, 0), (n_row0 - 1, 0, 0, 0), (0, 1, 0, 0))]

    def greet_near(sem):
        for step in near:
            pl.semaphore_signal(
                sem, inc=1, device_id=peer(step), device_id_type=MESH
            )

    start_load(0)
    for axis in range(2):
        for to in (1, -1):
            pl.semaphore_signal(
                barrier, inc=1, device_id=neighbour(axis, to), device_id_type=MESH
            )
    greet_near(barrier)
    col_part[...] = jnp.zeros_like(col_part)
    row_part[:, rows - 2 * CHUNK :, :] = jnp.zeros(
        (mats, 2 * CHUNK, LANES), jnp.float32
    )
    row_copy.start()
    col_copy.start()
    load(0, 0).wait()
    prepare_relay(0, 0)
    pl.semaphore_wait(barrier, 4 + len(near))
    send_relay(0, 0)
    load(0, 1).wait()
    prepare_relay(0, 1)
    send_relay(0, 1)
    for k in range(1, 1 + X_AHEAD):
        start_load(k)
    for color in range(2):
        prepare_direct(0, color)
        send_direct(0, color)
    greet_near(greet.at[0])
    row_copy.wait()
    col_copy.wait()

    def step(it, _):
        @pl.when(it > 0)
        def _():
            stage0(it)

            @pl.when(it + X_AHEAD < chunks)
            def _():
                start_load(it + X_AHEAD)

        for lag, work, end in (
            (3, stage2_direct, per_mat),
            (1, stage1, chunks),
            (2, stage2, chunks),
            (3, stage3, chunks),
            (4, stage4, per_mat),
        ):

            @pl.when((it >= lag) & (it < end + lag))
            def _():
                work(it - lag)

        @pl.when(it + 1 < chunks)
        def _():
            prepare(it + 1)

        @pl.when(it == 1)
        def _():
            pl.semaphore_wait(greet.at[0], len(near))
            greet_near(greet.at[1])

        @pl.when(it == 2)
        def _():
            pl.semaphore_wait(greet.at[1], len(near))

        for when, work in (
            (per_mat + 3, share_early),
            (per_mat + 3, share_sums),
            (per_mat + 5, share_clip),
            (per_mat + 7, finish),
        ):

            @pl.when(it == when)
            def _():
                work(0)

        return 0

    lax.fori_loop(0, chunks, step, 0)

    def direct(first, count):
        def one(k, _):
            stage2_direct(k)
            return 0

        lax.fori_loop(first, first + count, one, 0)

    last = chunks - 1
    share = per_mat // 4
    stage1(last)
    direct(per_mat, share)
    stage2(last - 1)
    stage3(last - 2)
    direct(per_mat + share, share)
    stage2(last)
    direct(per_mat + 2 * share, share)
    stage3(last - 1)
    direct(per_mat + 3 * share, per_mat - 3 * share)
    stage3(last)

    def finish_chunk(k, _):
        stage4(k)
        return 0

    lax.fori_loop(per_mat, last, finish_chunk, 0)
    share_early(mats - 1)
    stage4(last)
    share_sums(mats - 1)
    share_clip(mats - 1)
    finish(mats - 1)

    for color in range(2):
        for slot in range(S_SLOTS):
            wait_bytes(stage.at[slot, color], send0.at[slot, color])
        wait_bytes(land1.at[:, color], send1.at[color])
        wait_bytes(land2.at[:, color], send2.at[color])
        wait_bytes(land2.at[:, color], send3.at[color])
        wait_bytes(land2.at[:, color], send5.at[color])


def finish_kernel(
    scaled, factor, new_rows, new_cols, update_hbm, rows_hbm, cols_hbm, out, sems
):
    mats, rows, width = scaled.shape
    pieces = 4
    last = mats - 1
    size = rows // pieces
    copies = []

    def start(src, dst):
        copy = pltpu.make_async_copy(src, dst, sems.at[len(copies)])
        copy.start()
        copies.append(copy)

    for m in range(last):
        start(scaled.at[m], update_hbm.at[m])
    scale = jnp.broadcast_to(factor[last][:, :1], (TILE, width))
    for p in range(pieces):
        for t in range(p * size, (p + 1) * size, TILE):
            r = slice(t, t + TILE)
            out[r, :] = scaled[last, r, :] * scale
        here = pl.ds(p * size, size)
        start(out.at[here], update_hbm.at[last, here])
    start(new_rows, rows_hbm)
    start(new_cols, cols_hbm)
    for copy in copies:
        copy.wait()


def on_device(grad_terms, row_moment, col_moment):
    _, mats, rows, _ = grad_terms.shape
    width = col_moment.shape[1]
    n_row = lax.axis_size("row_0") * lax.axis_size("row_1")
    n_col = RING * RING
    chunks = mats * rows // (2 * CHUNK)
    f32 = jnp.float32
    vmem = pl.BlockSpec(memory_space=pltpu.VMEM)
    hbm = pl.BlockSpec(memory_space=pltpu.HBM)
    dma = pltpu.SemaphoreType.DMA
    shapes = (
        jax.ShapeDtypeStruct((mats, rows, width), f32),
        jax.ShapeDtypeStruct((mats, TILE, LANES), f32),
        jax.ShapeDtypeStruct((mats, rows), f32),
        jax.ShapeDtypeStruct((mats, width), f32),
    )
    scaled, factor, new_rows, new_cols = pl.pallas_call(
        kernel,
        out_shape=shapes,
        in_specs=[hbm, hbm, hbm],
        out_specs=(vmem, vmem, vmem, vmem),
        scratch_shapes=[
            pltpu.VMEM((X_SLOTS, 2, CHUNK, n_col * width), jnp.bfloat16),
            pltpu.VMEM((S_SLOTS, 2, 4, HALF, RING * width), f32),
            pltpu.VMEM((chunks, 2, 2, HALF, RING * width), f32),
            pltpu.VMEM((chunks, 2, 4, HALF, RING * width), f32),
            pltpu.VMEM((chunks, 2, 2, HALF, width), f32),
            pltpu.VMEM((chunks, 2, 4, HALF, width), f32),
            pltpu.VMEM((mats, rows), f32),
            pltpu.VMEM((mats, width), f32),
            pltpu.VMEM((mats, rows, LANES), f32),
            pltpu.VMEM((mats, TILE, width), f32),
            pltpu.VMEM((rows, LANES), f32),
            pltpu.VMEM((rows // LANES, LANES), f32),
            pltpu.VMEM((rows, LANES), f32),
            pltpu.VMEM((mats, n_col, rows // LANES, LANES), f32),
            pltpu.VMEM((mats, n_row, 1, width), f32),
            pltpu.VMEM((mats, n_row * n_col, 2, LANES), f32),
            pltpu.VMEM((mats, n_col, 1, LANES), f32),
            pltpu.VMEM((n_row, LANES), f32),
            dma((X_SLOTS, 2)),
            dma((2,)),
            dma((S_SLOTS, 2)),
            dma((2,)),
            dma((2,)),
            dma((2,)),
            dma((2,)),
            dma((R_SLOTS, 2)),
            dma((R_SLOTS, 2)),
            dma((R_SLOTS, 2)),
            dma((chunks,)),
            pltpu.SemaphoreType.REGULAR((2,)),
            dma((mats, 4)),
            dma((mats, 4)),
        ],
        compiler_params=pltpu.CompilerParams(
            collective_id=0,
            has_side_effects=True,
            vmem_limit_bytes=50 * 1024 * 1024,
        ),
    )(
        grad_terms,
        pltpu.with_memory_space_constraint(row_moment, pltpu.HBM),
        pltpu.with_memory_space_constraint(col_moment, pltpu.HBM),
    )
    return pl.pallas_call(
        finish_kernel,
        out_shape=(shapes[0], shapes[2], shapes[3]),
        in_specs=[vmem] * 4,
        out_specs=(hbm, hbm, hbm),
        scratch_shapes=[pltpu.VMEM((rows, width), f32), dma((8,))],
        compiler_params=pltpu.CompilerParams(vmem_limit_bytes=4 * 1024 * 1024),
    )(scaled, factor, new_rows, new_cols)


def solution(mesh):
    n_row = mesh.shape["row"]
    core = 2 if n_row > 1 else 1
    torus = Mesh(
        mesh.devices.reshape(n_row // core, core, RING, RING), ROW + COL
    )
    in_specs = (P(COL, None, ROW, None), P(None, ROW), P(None, COL))
    out_specs = (P(None, ROW, COL), P(None, ROW), P(None, COL))
    return jax.shard_map(
        on_device, mesh=torus, in_specs=in_specs, out_specs=out_specs, check_vma=False
    )
```

```python
import functools

import jax
import jax.numpy as jnp
from jax import lax
from jax.experimental import pallas as pl
from jax.experimental.pallas import tpu as pltpu
from jax.sharding import Mesh
from jax.sharding import PartitionSpec as P

MESH = pl.DeviceIdType.MESH
COL = ("col_0", "col_1")
ROW = ("row_0", "row_1")
RING = 4
LANES = 128
HALF = 16
CHUNK = 2 * HALF
X_SLOTS = 5
X_AHEAD = 2
S_SLOTS = 3
TILE = 8
R_SLOTS = 5

second_decay = 1.0 - 100.0 ** (-0.8)
tiny_square = 1e-30


def far_first(n_z, n_core):
    def hops(step, n):
        return min(step, n - step)

    steps = [
        (z, core, x, y)
        for z in range(n_z)
        for core in range(n_core)
        for x in range(RING)
        for y in range(RING)
    ]
    steps.sort(
        key=lambda s: -(hops(s[0], n_z) + hops(s[2], RING) + hops(s[3], RING))
    )
    return [s for s in steps if any(s)]


def wait_bytes(ref, sem):
    pltpu.make_async_copy(ref, ref, sem).wait()


def kernel(
    grad_hbm,
    row_hbm,
    col_hbm,
    update,
    factor,
    new_rows,
    new_cols,
    x_in,
    stage,
    land1,
    sum1,
    land2,
    sum2,
    row_moment,
    col_moment,
    row_part,
    col_part,
    weighted,
    weighted_row,
    row_scale,
    row_land,
    col_land,
    all_land,
    late_land,
    late_all,
    x_sem,
    m_sem,
    send0,
    send1,
    send2,
    send3,
    send5,
    recv1,
    recv2,
    recv3,
    recv4,
    greet,
    stat_send,
    stat_recv,
):
    mats, rows = row_moment.shape
    offsets = far_first(lax.axis_size("row_0"), lax.axis_size("row_1"))
    width = col_moment.shape[1]
    block = RING * width
    row_groups = rows // LANES
    n_row0, n_row1 = lax.axis_size("row_0"), lax.axis_size("row_1")
    n_row, n_col = n_row0 * n_row1, RING * RING
    total_rows = n_row * rows
    total_cols = n_col * width
    per_mat = rows // (2 * CHUNK)
    chunks = mats * per_mat

    here = (lax.axis_index("col_0"), lax.axis_index("col_1"))
    my_col = here[0] * RING + here[1]
    my_row = lax.axis_index("row_0") * n_row1 + lax.axis_index("row_1")

    def at(axis, step):
        return lax.rem(here[axis] + (step + RING), RING)

    me = my_row * n_col + my_col

    def neighbour(axis, step):
        return {COL[axis]: at(axis, step)}

    def col_peer(d):
        t = lax.rem(my_col + d, n_col)
        return {"col_0": t // RING, "col_1": lax.rem(t, RING)}

    def row_peer(d):
        t = lax.rem(my_row + d, n_row)
        return {"row_0": t // n_row1, "row_1": lax.rem(t, n_row1)}

    def send(src, dst, s_sem, r_sem, device):
        pltpu.make_async_remote_copy(
            src_ref=src,
            dst_ref=dst,
            send_sem=s_sem,
            recv_sem=r_sem,
            device_id=device,
            device_id_type=MESH,
        ).start()

    def load(k, color, sem):
        slot = lax.rem(k, X_SLOTS)
        m = k // per_mat
        r = lax.rem(k, per_mat) * (2 * CHUNK) + color * CHUNK
        return pltpu.make_async_copy(
            grad_hbm.at[0, m, pl.ds(pl.multiple_of(r, CHUNK), CHUNK), :],
            x_in.at[slot, color],
            sem,
        )

    def start_load(k):
        for color in range(2):
            load(k, color, x_sem.at[lax.rem(k, X_SLOTS)]).start()

    def own(color, k, idx, seg):
        outer, inner = (idx, seg) if color == 0 else (seg, idx)
        c = pl.multiple_of(outer * block + inner * width, LANES)
        v = x_in[lax.rem(k, X_SLOTS), color, :, pl.ds(c, width)].astype(jnp.float32)
        return v[:HALF], v[HALF:]

    def cols(s):
        return slice(s * width, (s + 1) * width)

    def inner_cols(idx):
        return pl.ds(pl.multiple_of(idx * width, LANES), width)

    def free_stage(k):
        slot = lax.rem(k, S_SLOTS)

        @pl.when(k >= S_SLOTS)
        def _():
            wait_bytes(stage.at[slot], send0.at[slot])

    def prepare_relay(k, color):
        slot = lax.rem(k, S_SLOTS)
        for s in range(RING):
            top, low = own(color, k, at(color, 2), s)
            stage[slot, color, 0, :, cols(s)] = top
            stage[slot, color, 1, :, cols(s)] = low

    def prepare_direct(k, color):
        slot = lax.rem(k, S_SLOTS)
        for s in range(RING):
            _, low = own(color, k, at(color, 1), s)
            stage[slot, color, 2, :, cols(s)] = low
            top, _ = own(color, k, at(color, -1), s)
            stage[slot, color, 3, :, cols(s)] = top

    def prepare(k):
        slot = lax.rem(k, X_SLOTS)
        wait_bytes(x_in.at[slot], x_sem.at[slot])
        free_stage(k)
        for color in range(2):
            prepare_relay(k, color)
            prepare_direct(k, color)

    def send_relay(k, color):
        slot = lax.rem(k, S_SLOTS)
        for which, step in ((0, 1), (1, -1)):
            send(
                stage.at[slot, color, which],
                land1.at[k, color, which],
                send0.at[slot],
                recv1.at[lax.rem(k, R_SLOTS)],
                neighbour(color, step),
            )

    def send_direct(k, color):
        slot = lax.rem(k, S_SLOTS)
        for which, step in ((2, 1), (3, -1)):
            send(
                stage.at[slot, color, which],
                sum1.at[k, color, which],
                send0.at[slot],
                recv2.at[lax.rem(k, R_SLOTS)],
                neighbour(color, step),
            )

    def stage0(k):
        for color in range(2):
            send_relay(k, color)
        for color in range(2):
            send_direct(k, color)

    def stage1(k):
        wait_bytes(land1.at[k], recv1.at[lax.rem(k, R_SLOTS)])
        for color in range(2):
            axis = color

            for s in range(RING):
                top, _ = own(color, k, at(axis, 1), s)
                land1[k, color, 0, :, cols(s)] = land1[k, color, 0, :, cols(s)] + top
                _, low = own(color, k, at(axis, -1), s)
                land1[k, color, 1, :, cols(s)] = land1[k, color, 1, :, cols(s)] + low
            for which, step in ((0, 1), (1, -1)):
                send(
                    land1.at[k, color, which],
                    sum1.at[k, color, which],
                    send1.at[0],
                    recv2.at[lax.rem(k, R_SLOTS)],
                    neighbour(axis, step),
                )

    def stage2(k):
        wait_bytes(sum1.at[k], recv2.at[lax.rem(k, R_SLOTS)])
        for color in range(2):
            axis = color

            for s in range(RING):
                top, low = own(color, k, at(axis, 0), s)
                sum1[k, color, 0, :, cols(s)] = (
                    sum1[k, color, 0, :, cols(s)]
                    + sum1[k, color, 3, :, cols(s)]
                    + top
                )
                sum1[k, color, 1, :, cols(s)] = (
                    sum1[k, color, 1, :, cols(s)]
                    + sum1[k, color, 2, :, cols(s)]
                    + low
                )
            axis = 1 - color
            for which, step in ((0, 1), (1, -1)):
                send(
                    sum1.at[k, color, which, :, inner_cols(at(axis, 2))],
                    land2.at[k, color, which],
                    send2.at[0],
                    recv3.at[lax.rem(k, R_SLOTS)],
                    neighbour(axis, step),
                )

    def stage2_direct(k):
        for color in range(2):
            axis = 1 - color
            for half, which, step in ((1, 2, 1), (0, 3, -1)):
                send(
                    sum1.at[k, color, half, :, inner_cols(at(axis, step))],
                    sum2.at[k, color, which],
                    send5.at[0],
                    recv4.at[k],
                    neighbour(axis, step),
                )

    def stage3(k):
        wait_bytes(land2.at[k], recv3.at[lax.rem(k, R_SLOTS)])
        for color in range(2):
            axis = 1 - color

            for which, step in ((0, 1), (1, -1)):
                land2[k, color, which] = (
                    land2[k, color, which]
                    + sum1[k, color, which, :, inner_cols(at(axis, step))]
                )
                send(
                    land2.at[k, color, which],
                    sum2.at[k, color, which],
                    send3.at[0],
                    recv4.at[k],
                    neighbour(axis, step),
                )

    def lane_tiles(v):
        out = v[:, :LANES]
        for c in range(1, width // LANES):
            out = out + v[:, c * LANES : (c + 1) * LANES]
        return out

    def stage4(k):
        m = k // per_mat
        r = lax.rem(k, per_mat) * (2 * CHUNK)
        squares_sum = col_part[m]
        wait_bytes(sum2.at[k], recv4.at[k])
        for color in range(2):
            axis = 1 - color
            for half, other in ((0, 3), (1, 2)):
                g = (
                    sum2[k, color, half]
                    + sum2[k, color, other]
                    + sum1[k, color, half, :, inner_cols(at(axis, 0))]
                )
                here_rows = pl.ds(
                    pl.multiple_of(r + color * CHUNK + half * HALF, HALF), HALF
                )
                update[m, here_rows, :] = g
                squares = g * g + tiny_square
                row_part[m, here_rows, :] = lane_tiles(squares)
                for t in range(HALF // TILE):
                    squares_sum = squares_sum + squares[t * TILE : (t + 1) * TILE]
        col_part[m] = squares_sum

    def pick(ref, m, lanes):
        return jnp.where(m == 0, ref[0:1, lanes], ref[1:2, lanes])

    def put(ref, m, lanes, value):
        for i in range(mats):

            @pl.when(m == i)
            def _():
                ref[i : i + 1, lanes] = value

    lane = lax.broadcasted_iota(jnp.int32, (1, LANES), 1)
    is_early = lane < LANES - 2 * CHUNK
    assert 2 * CHUNK == LANES // 2

    def lane_major(part):
        return jnp.sum(part.T, axis=0, keepdims=True)

    def group(b):
        return slice(b * LANES, (b + 1) * LANES)

    def peer(step):
        z, core, x, y = step
        there = {}
        if z or core:
            there["row_0"] = lax.rem(lax.axis_index("row_0") + z, n_row0)
            there["row_1"] = lax.rem(lax.axis_index("row_1") + core, n_row1)
        if x or y:
            there["col_0"] = at(0, x)
            there["col_1"] = at(1, y)
        return there

    def to_cols(m, buf, which):
        mine = buf.at[m, my_col]
        for step in offsets:
            if not any(step[:2]):
                send(
                    mine, mine, stat_send.at[which], stat_recv.at[m, which], peer(step)
                )

    def share_early(m):
        for b in range(row_groups):
            row_land[m, my_col, b : b + 1, :] = lane_major(row_part[m, group(b), :])
        to_cols(m, row_land, 1)

    def share_sums(m):
        col_land[m, my_row] = jnp.sum(col_part[m], axis=0, keepdims=True)
        mine = col_land.at[m, my_row]
        for step in offsets:
            if not any(step[2:]):
                send(mine, mine, stat_send.at[0], stat_recv.at[m, 0], peer(step))
        late_land[m, my_col] = lane_major(row_part[m, group(row_groups - 1), :])
        to_cols(m, late_land, 3)

    def all_but_one(m, buf, sem, n):
        if n > 1:
            wait_bytes(buf.at[m, pl.ds(0, n - 1)], sem)

    def share_clip(m):
        all_but_one(m, col_land, stat_recv.at[m, 0], n_row)
        full = col_land[m, 0]
        for s in range(1, n_row):
            full = full + col_land[m, s]
        col = (
            second_decay * pick(col_moment, m, slice(None))
            + (1.0 - second_decay) * full / total_rows
        )
        inverse = jnp.broadcast_to(1.0 / col, (TILE, width))

        def weigh(t, _):
            r = pl.ds(pl.multiple_of(t * TILE, TILE), TILE)
            v = update[m, r, :]
            weighted[r, :] = lane_tiles(v * v * inverse)
            return 0

        lax.fori_loop(0, rows // TILE, weigh, 0, unroll=8)
        for b in range(row_groups):
            weighted_row[b : b + 1, :] = lane_major(weighted[group(b), :])

        all_but_one(m, row_land, stat_recv.at[m, 1], n_col)
        full = row_land[m, 0]
        for s in range(1, n_col):
            full = full + row_land[m, s]
        moments, clip, level = [], None, None
        for b in range(row_groups):
            moment = (
                second_decay * pick(row_moment, m, group(b))
                + (1.0 - second_decay) * full[b : b + 1] / total_cols
            )
            moments.append(moment)
            part = weighted_row[b : b + 1, :] / moment
            if b == row_groups - 1:
                part = jnp.where(is_early, part, 0.0)
                moment = jnp.where(is_early, moment, 0.0)
            clip = part if clip is None else clip + part
            level = moment if level is None else level + moment
        clip = clip + pltpu.roll(clip, LANES // 2, 1)
        level = level + pltpu.roll(level, LANES // 2, 1)
        late = (
            second_decay * pick(row_moment, m, group(row_groups - 1)) / n_col
            + (1.0 - second_decay) * late_land[m, my_col] / total_cols
        )
        late_weight = pltpu.roll(
            weighted_row[row_groups - 1 : row_groups, :], LANES // 2, 1
        )
        all_land[m, me, 0:1, :] = jnp.where(is_early, clip, level)
        all_land[m, me, 1:2, :] = jnp.where(is_early, late_weight, late)
        mine = all_land.at[m, me]
        for step in offsets:
            send(mine, mine, stat_send.at[2], stat_recv.at[m, 2], peer(step))
        put(new_cols, m, slice(None), col)
        col_scale = jnp.broadcast_to(lax.rsqrt(col), (TILE, width))

        def rescale(t, _):
            r = pl.ds(pl.multiple_of(t * TILE, TILE), TILE)
            scale = row_scale[r, :]
            for c in range(width // LANES):
                lanes = group(c)
                update[m, r, lanes] = update[m, r, lanes] * col_scale[:, lanes] * scale
            return 0

        for b in range(row_groups - 1):
            put(new_rows, m, group(b), moments[b])
            row_scale[group(b), :] = jnp.broadcast_to(
                lax.rsqrt(moments[b]), (LANES, LANES)
            ).T
        tiles = (row_groups - 1) * LANES // TILE
        lax.fori_loop(0, tiles, rescale, 0, unroll=8)

        all_but_one(m, late_land, stat_recv.at[m, 3], n_col)
        full = late_land[m, 0]
        for s in range(1, n_col):
            full = full + late_land[m, s]
        b = row_groups - 1
        moment = (
            second_decay * pick(row_moment, m, group(b))
            + (1.0 - second_decay) * full / total_cols
        )
        moment = jnp.where(is_early, moments[b], moment)
        put(new_rows, m, group(b), moment)
        row_scale[group(b), :] = jnp.broadcast_to(lax.rsqrt(moment), (LANES, LANES)).T
        lax.fori_loop(tiles, rows // TILE, rescale, 0, unroll=8)

    def finish(m):
        all_but_one(m, all_land, stat_recv.at[m, 2], n_row * n_col)
        total = None
        for r in range(n_row):
            parts = [all_land[m, r * n_col + c] for c in range(4)]
            for c in range(4, n_col):
                parts[c % 4] = parts[c % 4] + all_land[m, r * n_col + c]
            one_row = (parts[0] + parts[1]) + (parts[2] + parts[3])
            total = one_row if total is None else total + one_row
            late_all[r : r + 1, :] = one_row[1:2]
        late = late_all[...]
        ratio = late / pltpu.roll(late, LANES // 2, 1)
        clip = jnp.where(is_early, total[0:1], 0.0) + jnp.sum(
            jnp.where(is_early, ratio, 0.0), axis=0, keepdims=True
        )
        level = jnp.where(is_early, 0.0, total[0:1] / n_col + total[1:2])
        clip = jnp.sum(clip, axis=1, keepdims=True)
        level = jnp.sum(level, axis=1, keepdims=True) / total_rows
        clip_scale = jnp.maximum(
            1.0, jnp.sqrt(clip * level / (total_rows * total_cols))
        )
        scale = jnp.broadcast_to(jnp.sqrt(level) / clip_scale, (TILE, LANES))
        factor[m] = scale

        @pl.when(m < mats - 1)
        def _():
            wide = jnp.broadcast_to(scale[:, :1], (TILE, width))

            def one(t, _):
                r = pl.ds(pl.multiple_of(t * TILE, TILE), TILE)
                update[m, r, :] = update[m, r, :] * wide
                return 0

            lax.fori_loop(0, rows // TILE, one, 0, unroll=4)

        all_but_one(m, col_land, stat_send.at[0], n_row)
        all_but_one(m, row_land, stat_send.at[1], n_col)
        all_but_one(m, all_land, stat_send.at[2], n_row * n_col)
        all_but_one(m, late_land, stat_send.at[3], n_col)

    barrier = pltpu.get_barrier_semaphore()
    row_copy = pltpu.make_async_copy(row_hbm, row_moment, m_sem.at[0])
    col_copy = pltpu.make_async_copy(col_hbm, col_moment, m_sem.at[1])

    near = [t for t in offsets if not any(t[2:])]
    near = [t for t in near if t in ((1, 0, 0, 0), (n_row0 - 1, 0, 0, 0), (0, 1, 0, 0))]

    def greet_near(sem):
        for step in near:
            pl.semaphore_signal(
                sem, inc=1, device_id=peer(step), device_id_type=MESH
            )

    first = [load(0, color, m_sem.at[2 + color]) for color in range(2)]
    for copy in first:
        copy.start()
    for axis in range(2):
        for to in (1, -1):
            pl.semaphore_signal(
                barrier, inc=1, device_id=neighbour(axis, to), device_id_type=MESH
            )
    greet_near(barrier)
    col_part[...] = jnp.zeros_like(col_part)
    row_part[:, rows - 2 * CHUNK :, :] = jnp.zeros(
        (mats, 2 * CHUNK, LANES), jnp.float32
    )
    row_copy.start()
    col_copy.start()
    first[0].wait()
    prepare_relay(0, 0)
    pl.semaphore_wait(barrier, 4 + len(near))
    send_relay(0, 0)
    first[1].wait()
    prepare_relay(0, 1)
    send_relay(0, 1)
    for k in range(1, 1 + X_AHEAD):
        start_load(k)
    for color in range(2):
        prepare_direct(0, color)
        send_direct(0, color)
    greet_near(greet.at[0])
    row_copy.wait()
    col_copy.wait()

    def step(it, _):
        @pl.when(it > 0)
        def _():
            stage0(it)

            @pl.when(it + X_AHEAD < chunks)
            def _():
                start_load(it + X_AHEAD)

        for lag, work, end in (
            (3, stage2_direct, per_mat),
            (1, stage1, chunks),
            (2, stage2, chunks),
            (3, stage3, chunks),
            (4, stage4, per_mat),
        ):

            @pl.when((it >= lag) & (it < end + lag))
            def _():
                work(it - lag)

        @pl.when(it + 1 < chunks)
        def _():
            prepare(it + 1)

        @pl.when(it == 1)
        def _():
            pl.semaphore_wait(greet.at[0], len(near))
            greet_near(greet.at[1])

        @pl.when(it == 2)
        def _():
            pl.semaphore_wait(greet.at[1], len(near))

        for when, work in (
            (per_mat + 3, share_early),
            (per_mat + 3, share_sums),
            (per_mat + 5, share_clip),
            (per_mat + 7, finish),
        ):

            @pl.when(it == when)
            def _():
                work(0)

        return 0

    lax.fori_loop(0, chunks, step, 0)

    def direct(first, count):
        def one(k, _):
            stage2_direct(k)
            return 0

        lax.fori_loop(first, first + count, one, 0)

    last = chunks - 1
    share = per_mat // 4
    stage1(last)
    direct(per_mat, share)
    stage2(last - 1)
    stage3(last - 2)
    direct(per_mat + share, share)
    stage2(last)
    direct(per_mat + 2 * share, share)
    stage3(last - 1)
    direct(per_mat + 3 * share, per_mat - 3 * share)
    stage3(last)

    def finish_chunk(k, _):
        stage4(k)
        return 0

    lax.fori_loop(per_mat, last, finish_chunk, 0)
    share_early(mats - 1)
    stage4(last)
    share_sums(mats - 1)
    share_clip(mats - 1)
    finish(mats - 1)

    for slot in range(S_SLOTS):
        wait_bytes(stage.at[slot], send0.at[slot])
    wait_bytes(land1, send1.at[0])
    wait_bytes(land2, send2.at[0])
    wait_bytes(land2, send3.at[0])
    wait_bytes(land2, send5.at[0])


def finish_kernel(
    scaled, factor, new_rows, new_cols, update_hbm, rows_hbm, cols_hbm, out, sems
):
    mats, rows, width = scaled.shape
    pieces = 4
    last = mats - 1
    size = rows // pieces
    copies = []

    def start(src, dst):
        copy = pltpu.make_async_copy(src, dst, sems.at[len(copies)])
        copy.start()
        copies.append(copy)

    for m in range(last):
        start(scaled.at[m], update_hbm.at[m])
    scale = jnp.broadcast_to(factor[last][:, :1], (TILE, width))
    for p in range(pieces):
        for t in range(p * size, (p + 1) * size, TILE):
            r = slice(t, t + TILE)
            out[r, :] = scaled[last, r, :] * scale
        here = pl.ds(p * size, size)
        start(out.at[here], update_hbm.at[last, here])
    start(new_rows, rows_hbm)
    start(new_cols, cols_hbm)
    for copy in copies:
        copy.wait()


def on_device(grad_terms, row_moment, col_moment):
    _, mats, rows, _ = grad_terms.shape
    width = col_moment.shape[1]
    n_row = lax.axis_size("row_0") * lax.axis_size("row_1")
    n_col = RING * RING
    chunks = mats * rows // (2 * CHUNK)
    f32 = jnp.float32
    vmem = pl.BlockSpec(memory_space=pltpu.VMEM)
    hbm = pl.BlockSpec(memory_space=pltpu.HBM)
    dma = pltpu.SemaphoreType.DMA
    shapes = (
        jax.ShapeDtypeStruct((mats, rows, width), f32),
        jax.ShapeDtypeStruct((mats, TILE, LANES), f32),
        jax.ShapeDtypeStruct((mats, rows), f32),
        jax.ShapeDtypeStruct((mats, width), f32),
    )
    scaled, factor, new_rows, new_cols = pl.pallas_call(
        kernel,
        out_shape=shapes,
        in_specs=[hbm, hbm, hbm],
        out_specs=(vmem, vmem, vmem, vmem),
        scratch_shapes=[
            pltpu.VMEM((X_SLOTS, 2, CHUNK, n_col * width), jnp.bfloat16),
            pltpu.VMEM((S_SLOTS, 2, 4, HALF, RING * width), f32),
            pltpu.VMEM((chunks, 2, 2, HALF, RING * width), f32),
            pltpu.VMEM((chunks, 2, 4, HALF, RING * width), f32),
            pltpu.VMEM((chunks, 2, 2, HALF, width), f32),
            pltpu.VMEM((chunks, 2, 4, HALF, width), f32),
            pltpu.VMEM((mats, rows), f32),
            pltpu.VMEM((mats, width), f32),
            pltpu.VMEM((mats, rows, LANES), f32),
            pltpu.VMEM((mats, TILE, width), f32),
            pltpu.VMEM((rows, LANES), f32),
            pltpu.VMEM((rows // LANES, LANES), f32),
            pltpu.VMEM((rows, LANES), f32),
            pltpu.VMEM((mats, n_col, rows // LANES, LANES), f32),
            pltpu.VMEM((mats, n_row, 1, width), f32),
            pltpu.VMEM((mats, n_row * n_col, 2, LANES), f32),
            pltpu.VMEM((mats, n_col, 1, LANES), f32),
            pltpu.VMEM((n_row, LANES), f32),
            dma((X_SLOTS,)),
            dma((4,)),
            dma((S_SLOTS,)),
            dma((1,)),
            dma((1,)),
            dma((1,)),
            dma((1,)),
            dma((R_SLOTS,)),
            dma((R_SLOTS,)),
            dma((R_SLOTS,)),
            dma((chunks,)),
            pltpu.SemaphoreType.REGULAR((2,)),
            dma((4,)),
            dma((mats, 4)),
        ],
        compiler_params=pltpu.CompilerParams(
            collective_id=0,
            has_side_effects=True,
            vmem_limit_bytes=50 * 1024 * 1024,
        ),
    )(
        grad_terms,
        pltpu.with_memory_space_constraint(row_moment, pltpu.HBM),
        pltpu.with_memory_space_constraint(col_moment, pltpu.HBM),
    )
    return pl.pallas_call(
        finish_kernel,
        out_shape=(shapes[0], shapes[2], shapes[3]),
        in_specs=[vmem] * 4,
        out_specs=(hbm, hbm, hbm),
        scratch_shapes=[pltpu.VMEM((rows, width), f32), dma((8,))],
        compiler_params=pltpu.CompilerParams(vmem_limit_bytes=4 * 1024 * 1024),
    )(scaled, factor, new_rows, new_cols)


def solution(mesh):
    n_row = mesh.shape["row"]
    core = 2 if n_row > 1 else 1
    torus = Mesh(
        mesh.devices.reshape(n_row // core, core, RING, RING), ROW + COL
    )
    in_specs = (P(COL, None, ROW, None), P(None, ROW), P(None, COL))
    out_specs = (P(None, ROW, COL), P(None, ROW), P(None, COL))
    return jax.shard_map(
        on_device, mesh=torus, in_specs=in_specs, out_specs=out_specs, check_vma=False
    )
```

```python
import functools

import jax
import jax.numpy as jnp
from jax import lax
from jax.experimental import pallas as pl
from jax.experimental.pallas import tpu as pltpu
from jax.sharding import Mesh
from jax.sharding import PartitionSpec as P

MESH = pl.DeviceIdType.MESH
COL = ("col_0", "col_1")
ROW = ("row_0", "row_1")
RING = 4
LANES = 128
HALF = 16
CHUNK = 2 * HALF
X_SLOTS = 5
X_AHEAD = 2
S_SLOTS = 3
TILE = 8
R_SLOTS = 5

second_decay = 1.0 - 100.0 ** (-0.8)
tiny_square = 1e-30


def far_first(n_z, n_core):
    def hops(step, n):
        return min(step, n - step)

    steps = [
        (z, core, x, y)
        for z in range(n_z)
        for core in range(n_core)
        for x in range(RING)
        for y in range(RING)
    ]
    steps.sort(
        key=lambda s: -(hops(s[0], n_z) + hops(s[2], RING) + hops(s[3], RING))
    )
    return [s for s in steps if any(s)]


def wait_bytes(ref, sem):
    pltpu.make_async_copy(ref, ref, sem).wait()


def kernel(
    grad_hbm,
    row_hbm,
    col_hbm,
    update,
    factor,
    new_rows,
    new_cols,
    x_in,
    stage,
    land1,
    sum1,
    land2,
    sum2,
    row_moment,
    col_moment,
    row_part,
    col_part,
    weighted,
    weighted_row,
    row_scale,
    row_land,
    col_land,
    all_land,
    late_land,
    late_all,
    x_sem,
    m_sem,
    send0,
    send1,
    send2,
    send3,
    send5,
    recv1,
    recv2,
    recv3,
    recv4,
    greet,
    stat_send,
    stat_recv,
):
    mats, rows = row_moment.shape
    offsets = far_first(lax.axis_size("row_0"), lax.axis_size("row_1"))
    width = col_moment.shape[1]
    block = RING * width
    row_groups = rows // LANES
    n_row0, n_row1 = lax.axis_size("row_0"), lax.axis_size("row_1")
    n_row, n_col = n_row0 * n_row1, RING * RING
    total_rows = n_row * rows
    total_cols = n_col * width
    per_mat = rows // (2 * CHUNK)
    chunks = mats * per_mat

    here = (lax.axis_index("col_0"), lax.axis_index("col_1"))
    my_col = here[0] * RING + here[1]
    my_row = lax.axis_index("row_0") * n_row1 + lax.axis_index("row_1")

    def at(axis, step):
        return lax.rem(here[axis] + (step + RING), RING)

    me = my_row * n_col + my_col

    def neighbour(axis, step):
        return {COL[axis]: at(axis, step)}

    def col_peer(d):
        t = lax.rem(my_col + d, n_col)
        return {"col_0": t // RING, "col_1": lax.rem(t, RING)}

    def row_peer(d):
        t = lax.rem(my_row + d, n_row)
        return {"row_0": t // n_row1, "row_1": lax.rem(t, n_row1)}

    def send(src, dst, s_sem, r_sem, device):
        pltpu.make_async_remote_copy(
            src_ref=src,
            dst_ref=dst,
            send_sem=s_sem,
            recv_sem=r_sem,
            device_id=device,
            device_id_type=MESH,
        ).start()

    def load(k, color, sem):
        slot = lax.rem(k, X_SLOTS)
        m = k // per_mat
        r = lax.rem(k, per_mat) * (2 * CHUNK) + color * CHUNK
        return pltpu.make_async_copy(
            grad_hbm.at[0, m, pl.ds(pl.multiple_of(r, CHUNK), CHUNK), :],
            x_in.at[slot, color],
            sem,
        )

    def start_load(k):
        for color in range(2):
            load(k, color, x_sem.at[lax.rem(k, X_SLOTS)]).start()

    def own(color, k, idx, seg):
        outer, inner = (idx, seg) if color == 0 else (seg, idx)
        c = pl.multiple_of(outer * block + inner * width, LANES)
        v = x_in[lax.rem(k, X_SLOTS), color, :, pl.ds(c, width)].astype(jnp.float32)
        return v[:HALF], v[HALF:]

    def cols(s):
        return slice(s * width, (s + 1) * width)

    def inner_cols(idx):
        return pl.ds(pl.multiple_of(idx * width, LANES), width)

    def free_stage(k):
        slot = lax.rem(k, S_SLOTS)

        @pl.when(k >= S_SLOTS)
        def _():
            wait_bytes(stage.at[slot], send0.at[slot])

    def prepare_relay(k, color):
        slot = lax.rem(k, S_SLOTS)
        for s in range(RING):
            top, low = own(color, k, at(color, 2), s)
            stage[slot, color, 0, :, cols(s)] = top
            stage[slot, color, 1, :, cols(s)] = low

    def prepare_direct(k, color):
        slot = lax.rem(k, S_SLOTS)
        for s in range(RING):
            _, low = own(color, k, at(color, 1), s)
            stage[slot, color, 2, :, cols(s)] = low
            top, _ = own(color, k, at(color, -1), s)
            stage[slot, color, 3, :, cols(s)] = top

    def prepare(k):
        slot = lax.rem(k, X_SLOTS)
        wait_bytes(x_in.at[slot], x_sem.at[slot])
        free_stage(k)
        for color in range(2):
            prepare_relay(k, color)
            prepare_direct(k, color)

    def send_relay(k, color):
        slot = lax.rem(k, S_SLOTS)
        for which, step in ((0, 1), (1, -1)):
            send(
                stage.at[slot, color, which],
                land1.at[k, color, which],
                send0.at[slot],
                recv1.at[lax.rem(k, R_SLOTS)],
                neighbour(color, step),
            )

    def send_direct(k, color):
        slot = lax.rem(k, S_SLOTS)
        for which, step in ((2, 1), (3, -1)):
            send(
                stage.at[slot, color, which],
                sum1.at[k, color, which],
                send0.at[slot],
                recv2.at[lax.rem(k, R_SLOTS)],
                neighbour(color, step),
            )

    def stage0(k):
        for color in range(2):
            send_relay(k, color)
        for color in range(2):
            send_direct(k, color)

    def stage1(k):
        wait_bytes(land1.at[k], recv1.at[lax.rem(k, R_SLOTS)])
        for color in range(2):
            axis = color

            for s in range(RING):
                top, _ = own(color, k, at(axis, 1), s)
                land1[k, color, 0, :, cols(s)] = land1[k, color, 0, :, cols(s)] + top
                _, low = own(color, k, at(axis, -1), s)
                land1[k, color, 1, :, cols(s)] = land1[k, color, 1, :, cols(s)] + low
            for which, step in ((0, 1), (1, -1)):
                send(
                    land1.at[k, color, which],
                    sum1.at[k, color, which],
                    send1.at[0],
                    recv2.at[lax.rem(k, R_SLOTS)],
                    neighbour(axis, step),
                )

    def stage2(k):
        wait_bytes(sum1.at[k], recv2.at[lax.rem(k, R_SLOTS)])
        for color in range(2):
            axis = color

            for s in range(RING):
                top, low = own(color, k, at(axis, 0), s)
                sum1[k, color, 0, :, cols(s)] = (
                    sum1[k, color, 0, :, cols(s)]
                    + sum1[k, color, 3, :, cols(s)]
                    + top
                )
                sum1[k, color, 1, :, cols(s)] = (
                    sum1[k, color, 1, :, cols(s)]
                    + sum1[k, color, 2, :, cols(s)]
                    + low
                )
            axis = 1 - color
            for which, step in ((0, 1), (1, -1)):
                send(
                    sum1.at[k, color, which, :, inner_cols(at(axis, 2))],
                    land2.at[k, color, which],
                    send2.at[0],
                    recv3.at[lax.rem(k, R_SLOTS)],
                    neighbour(axis, step),
                )

    def stage2_direct(k):
        for color in range(2):
            axis = 1 - color
            for half, which, step in ((1, 2, 1), (0, 3, -1)):
                send(
                    sum1.at[k, color, half, :, inner_cols(at(axis, step))],
                    sum2.at[k, color, which],
                    send5.at[0],
                    recv4.at[lax.rem(k, per_mat)],
                    neighbour(axis, step),
                )

    def stage3(k):
        wait_bytes(land2.at[k], recv3.at[lax.rem(k, R_SLOTS)])
        for color in range(2):
            axis = 1 - color

            for which, step in ((0, 1), (1, -1)):
                land2[k, color, which] = (
                    land2[k, color, which]
                    + sum1[k, color, which, :, inner_cols(at(axis, step))]
                )
                send(
                    land2.at[k, color, which],
                    sum2.at[k, color, which],
                    send3.at[0],
                    recv4.at[lax.rem(k, per_mat)],
                    neighbour(axis, step),
                )

    def lane_tiles(v):
        out = v[:, :LANES]
        for c in range(1, width // LANES):
            out = out + v[:, c * LANES : (c + 1) * LANES]
        return out

    def stage4(k):
        m = k // per_mat
        r = lax.rem(k, per_mat) * (2 * CHUNK)
        squares_sum = col_part[m]
        wait_bytes(sum2.at[k], recv4.at[lax.rem(k, per_mat)])
        for color in range(2):
            axis = 1 - color
            for half, other in ((0, 3), (1, 2)):
                g = (
                    sum2[k, color, half]
                    + sum2[k, color, other]
                    + sum1[k, color, half, :, inner_cols(at(axis, 0))]
                )
                here_rows = pl.ds(
                    pl.multiple_of(r + color * CHUNK + half * HALF, HALF), HALF
                )
                update[m, here_rows, :] = g
                squares = g * g + tiny_square
                row_part[m, here_rows, :] = lane_tiles(squares)
                for t in range(HALF // TILE):
                    squares_sum = squares_sum + squares[t * TILE : (t + 1) * TILE]
        col_part[m] = squares_sum

    def pick(ref, m, lanes):
        return jnp.where(m == 0, ref[0:1, lanes], ref[1:2, lanes])

    def put(ref, m, lanes, value):
        for i in range(mats):

            @pl.when(m == i)
            def _():
                ref[i : i + 1, lanes] = value

    lane = lax.broadcasted_iota(jnp.int32, (1, LANES), 1)
    is_early = lane < LANES - 2 * CHUNK
    assert 2 * CHUNK == LANES // 2

    def lane_major(part):
        return jnp.sum(part.T, axis=0, keepdims=True)

    def group(b):
        return slice(b * LANES, (b + 1) * LANES)

    def peer(step):
        z, core, x, y = step
        there = {}
        if z or core:
            there["row_0"] = lax.rem(lax.axis_index("row_0") + z, n_row0)
            there["row_1"] = lax.rem(lax.axis_index("row_1") + core, n_row1)
        if x or y:
            there["col_0"] = at(0, x)
            there["col_1"] = at(1, y)
        return there

    def to_cols(m, buf, which):
        mine = buf.at[m, my_col]
        for step in offsets:
            if not any(step[:2]):
                send(
                    mine, mine, stat_send.at[which], stat_recv.at[m, which], peer(step)
                )

    def share_early(m):
        for b in range(row_groups):
            row_land[m, my_col, b : b + 1, :] = lane_major(row_part[m, group(b), :])
        to_cols(m, row_land, 1)

    def share_sums(m):
        col_land[m, my_row] = jnp.sum(col_part[m], axis=0, keepdims=True)
        mine = col_land.at[m, my_row]
        for step in offsets:
            if not any(step[2:]):
                send(mine, mine, stat_send.at[0], stat_recv.at[m, 0], peer(step))
        late_land[m, my_col] = lane_major(row_part[m, group(row_groups - 1), :])
        to_cols(m, late_land, 3)

    def all_but_one(m, buf, sem, n):
        if n > 1:
            wait_bytes(buf.at[m, pl.ds(0, n - 1)], sem)

    def share_clip(m):
        all_but_one(m, col_land, stat_recv.at[m, 0], n_row)
        full = col_land[m, 0]
        for s in range(1, n_row):
            full = full + col_land[m, s]
        col = (
            second_decay * pick(col_moment, m, slice(None))
            + (1.0 - second_decay) * full / total_rows
        )
        inverse = jnp.broadcast_to(1.0 / col, (TILE, width))

        def weigh(t, _):
            r = pl.ds(pl.multiple_of(t * TILE, TILE), TILE)
            v = update[m, r, :]
            weighted[r, :] = lane_tiles(v * v * inverse)
            return 0

        lax.fori_loop(0, rows // TILE, weigh, 0, unroll=8)
        for b in range(row_groups):
            weighted_row[b : b + 1, :] = lane_major(weighted[group(b), :])

        all_but_one(m, row_land, stat_recv.at[m, 1], n_col)
        full = row_land[m, 0]
        for s in range(1, n_col):
            full = full + row_land[m, s]
        moments, clip, level = [], None, None
        for b in range(row_groups):
            moment = (
                second_decay * pick(row_moment, m, group(b))
                + (1.0 - second_decay) * full[b : b + 1] / total_cols
            )
            moments.append(moment)
            part = weighted_row[b : b + 1, :] / moment
            if b == row_groups - 1:
                part = jnp.where(is_early, part, 0.0)
                moment = jnp.where(is_early, moment, 0.0)
            clip = part if clip is None else clip + part
            level = moment if level is None else level + moment
        clip = clip + pltpu.roll(clip, LANES // 2, 1)
        level = level + pltpu.roll(level, LANES // 2, 1)
        late = (
            second_decay * pick(row_moment, m, group(row_groups - 1)) / n_col
            + (1.0 - second_decay) * late_land[m, my_col] / total_cols
        )
        late_weight = pltpu.roll(
            weighted_row[row_groups - 1 : row_groups, :], LANES // 2, 1
        )
        all_land[m, me, 0:1, :] = jnp.where(is_early, clip, level)
        all_land[m, me, 1:2, :] = jnp.where(is_early, late_weight, late)
        mine = all_land.at[m, me]
        for step in offsets:
            send(mine, mine, stat_send.at[2], stat_recv.at[m, 2], peer(step))
        put(new_cols, m, slice(None), col)
        col_scale = jnp.broadcast_to(lax.rsqrt(col), (TILE, width))

        def rescale(t, _):
            r = pl.ds(pl.multiple_of(t * TILE, TILE), TILE)
            scale = row_scale[r, :]
            for c in range(width // LANES):
                lanes = group(c)
                update[m, r, lanes] = update[m, r, lanes] * col_scale[:, lanes] * scale
            return 0

        for b in range(row_groups - 1):
            put(new_rows, m, group(b), moments[b])
            row_scale[group(b), :] = jnp.broadcast_to(
                lax.rsqrt(moments[b]), (LANES, LANES)
            ).T
        tiles = (row_groups - 1) * LANES // TILE
        lax.fori_loop(0, tiles, rescale, 0, unroll=8)

        all_but_one(m, late_land, stat_recv.at[m, 3], n_col)
        full = late_land[m, 0]
        for s in range(1, n_col):
            full = full + late_land[m, s]
        b = row_groups - 1
        moment = (
            second_decay * pick(row_moment, m, group(b))
            + (1.0 - second_decay) * full / total_cols
        )
        moment = jnp.where(is_early, moments[b], moment)
        put(new_rows, m, group(b), moment)
        row_scale[group(b), :] = jnp.broadcast_to(lax.rsqrt(moment), (LANES, LANES)).T
        lax.fori_loop(tiles, rows // TILE, rescale, 0, unroll=8)

    def finish(m):
        all_but_one(m, all_land, stat_recv.at[m, 2], n_row * n_col)
        total = None
        for r in range(n_row):
            parts = [all_land[m, r * n_col + c] for c in range(4)]
            for c in range(4, n_col):
                parts[c % 4] = parts[c % 4] + all_land[m, r * n_col + c]
            one_row = (parts[0] + parts[1]) + (parts[2] + parts[3])
            total = one_row if total is None else total + one_row
            late_all[r : r + 1, :] = one_row[1:2]
        late = late_all[...]
        ratio = late / pltpu.roll(late, LANES // 2, 1)
        clip = jnp.where(is_early, total[0:1], 0.0) + jnp.sum(
            jnp.where(is_early, ratio, 0.0), axis=0, keepdims=True
        )
        level = jnp.where(is_early, 0.0, total[0:1] / n_col + total[1:2])
        clip = jnp.sum(clip, axis=1, keepdims=True)
        level = jnp.sum(level, axis=1, keepdims=True) / total_rows
        clip_scale = jnp.maximum(
            1.0, jnp.sqrt(clip * level / (total_rows * total_cols))
        )
        scale = jnp.broadcast_to(jnp.sqrt(level) / clip_scale, (TILE, LANES))
        factor[m] = scale

        @pl.when(m < mats - 1)
        def _():
            wide = jnp.broadcast_to(scale[:, :1], (TILE, width))

            def one(t, _):
                r = pl.ds(pl.multiple_of(t * TILE, TILE), TILE)
                update[m, r, :] = update[m, r, :] * wide
                return 0

            lax.fori_loop(0, rows // TILE, one, 0, unroll=4)

        all_but_one(m, col_land, stat_send.at[0], n_row)
        all_but_one(m, row_land, stat_send.at[1], n_col)
        all_but_one(m, all_land, stat_send.at[2], n_row * n_col)
        all_but_one(m, late_land, stat_send.at[3], n_col)

    barrier = pltpu.get_barrier_semaphore()
    row_copy = pltpu.make_async_copy(row_hbm, row_moment, m_sem.at[0])
    col_copy = pltpu.make_async_copy(col_hbm, col_moment, m_sem.at[1])

    near = [t for t in offsets if not any(t[2:])]
    near = [t for t in near if t in ((1, 0, 0, 0), (n_row0 - 1, 0, 0, 0), (0, 1, 0, 0))]

    def greet_near(sem):
        for step in near:
            pl.semaphore_signal(
                sem, inc=1, device_id=peer(step), device_id_type=MESH
            )

    first = [load(0, color, m_sem.at[2 + color]) for color in range(2)]
    for copy in first:
        copy.start()
    for axis in range(2):
        for to in (1, -1):
            pl.semaphore_signal(
                barrier, inc=1, device_id=neighbour(axis, to), device_id_type=MESH
            )
    greet_near(barrier)
    col_part[...] = jnp.zeros_like(col_part)
    row_part[:, rows - 2 * CHUNK :, :] = jnp.zeros(
        (mats, 2 * CHUNK, LANES), jnp.float32
    )
    row_copy.start()
    col_copy.start()
    first[0].wait()
    prepare_relay(0, 0)
    pl.semaphore_wait(barrier, 4 + len(near))
    send_relay(0, 0)
    first[1].wait()
    prepare_relay(0, 1)
    send_relay(0, 1)
    for k in range(1, 1 + X_AHEAD):
        start_load(k)
    for color in range(2):
        prepare_direct(0, color)
        send_direct(0, color)
    greet_near(greet.at[0])
    row_copy.wait()
    col_copy.wait()

    def step(it, _):
        @pl.when(it > 0)
        def _():
            stage0(it)

            @pl.when(it + X_AHEAD < chunks)
            def _():
                start_load(it + X_AHEAD)

        for lag, work, end in (
            (3, stage2_direct, per_mat),
            (1, stage1, chunks),
            (2, stage2, chunks),
            (3, stage3, chunks),
            (4, stage4, per_mat),
        ):

            @pl.when((it >= lag) & (it < end + lag))
            def _():
                work(it - lag)

        @pl.when(it + 1 < chunks)
        def _():
            prepare(it + 1)

        @pl.when(it == 1)
        def _():
            pl.semaphore_wait(greet.at[0], len(near))
            greet_near(greet.at[1])

        @pl.when(it == 2)
        def _():
            pl.semaphore_wait(greet.at[1], len(near))

        for when, work in (
            (per_mat + 3, share_early),
            (per_mat + 3, share_sums),
            (per_mat + 5, share_clip),
            (per_mat + 7, finish),
        ):

            @pl.when(it == when)
            def _():
                work(0)

        return 0

    lax.fori_loop(0, chunks, step, 0)

    def direct(first, count):
        def one(k, _):
            stage2_direct(k)
            return 0

        lax.fori_loop(first, first + count, one, 0)

    last = chunks - 1
    share = per_mat // 4
    stage1(last)
    direct(per_mat, share)
    stage2(last - 1)
    stage3(last - 2)
    direct(per_mat + share, share)
    stage2(last)
    direct(per_mat + 2 * share, share)
    stage3(last - 1)
    direct(per_mat + 3 * share, per_mat - 3 * share)
    stage3(last)

    def finish_chunk(k, _):
        stage4(k)
        return 0

    lax.fori_loop(per_mat, last, finish_chunk, 0)
    share_early(mats - 1)
    stage4(last)
    share_sums(mats - 1)
    share_clip(mats - 1)
    finish(mats - 1)

    for slot in range(S_SLOTS):
        wait_bytes(stage.at[slot], send0.at[slot])
    wait_bytes(land1, send1.at[0])
    wait_bytes(land2, send2.at[0])
    wait_bytes(land2, send3.at[0])
    wait_bytes(land2, send5.at[0])


def finish_kernel(
    scaled, factor, new_rows, new_cols, update_hbm, rows_hbm, cols_hbm, out, sems
):
    mats, rows, width = scaled.shape
    pieces = 4
    last = mats - 1
    size = rows // pieces
    copies = []

    def start(src, dst):
        copy = pltpu.make_async_copy(src, dst, sems.at[len(copies)])
        copy.start()
        copies.append(copy)

    for m in range(last):
        start(scaled.at[m], update_hbm.at[m])
    scale = jnp.broadcast_to(factor[last][:, :1], (TILE, width))
    for p in range(pieces):
        for t in range(p * size, (p + 1) * size, TILE):
            r = slice(t, t + TILE)
            out[r, :] = scaled[last, r, :] * scale
        here = pl.ds(p * size, size)
        start(out.at[here], update_hbm.at[last, here])
    start(new_rows, rows_hbm)
    start(new_cols, cols_hbm)
    for copy in copies:
        copy.wait()


def on_device(grad_terms, row_moment, col_moment):
    _, mats, rows, _ = grad_terms.shape
    width = col_moment.shape[1]
    n_row = lax.axis_size("row_0") * lax.axis_size("row_1")
    n_col = RING * RING
    chunks = mats * rows // (2 * CHUNK)
    f32 = jnp.float32
    vmem = pl.BlockSpec(memory_space=pltpu.VMEM)
    hbm = pl.BlockSpec(memory_space=pltpu.HBM)
    dma = pltpu.SemaphoreType.DMA
    shapes = (
        jax.ShapeDtypeStruct((mats, rows, width), f32),
        jax.ShapeDtypeStruct((mats, TILE, LANES), f32),
        jax.ShapeDtypeStruct((mats, rows), f32),
        jax.ShapeDtypeStruct((mats, width), f32),
    )
    scaled, factor, new_rows, new_cols = pl.pallas_call(
        kernel,
        out_shape=shapes,
        in_specs=[hbm, hbm, hbm],
        out_specs=(vmem, vmem, vmem, vmem),
        scratch_shapes=[
            pltpu.VMEM((X_SLOTS, 2, CHUNK, n_col * width), jnp.bfloat16),
            pltpu.VMEM((S_SLOTS, 2, 4, HALF, RING * width), f32),
            pltpu.VMEM((chunks, 2, 2, HALF, RING * width), f32),
            pltpu.VMEM((chunks, 2, 4, HALF, RING * width), f32),
            pltpu.VMEM((chunks, 2, 2, HALF, width), f32),
            pltpu.VMEM((chunks, 2, 4, HALF, width), f32),
            pltpu.VMEM((mats, rows), f32),
            pltpu.VMEM((mats, width), f32),
            pltpu.VMEM((mats, rows, LANES), f32),
            pltpu.VMEM((mats, TILE, width), f32),
            pltpu.VMEM((rows, LANES), f32),
            pltpu.VMEM((rows // LANES, LANES), f32),
            pltpu.VMEM((rows, LANES), f32),
            pltpu.VMEM((mats, n_col, rows // LANES, LANES), f32),
            pltpu.VMEM((mats, n_row, 1, width), f32),
            pltpu.VMEM((mats, n_row * n_col, 2, LANES), f32),
            pltpu.VMEM((mats, n_col, 1, LANES), f32),
            pltpu.VMEM((n_row, LANES), f32),
            dma((X_SLOTS,)),
            dma((4,)),
            dma((S_SLOTS,)),
            dma((1,)),
            dma((1,)),
            dma((1,)),
            dma((1,)),
            dma((R_SLOTS,)),
            dma((R_SLOTS,)),
            dma((R_SLOTS,)),
            dma((chunks // mats,)),
            pltpu.SemaphoreType.REGULAR((2,)),
            dma((4,)),
            dma((mats, 4)),
        ],
        compiler_params=pltpu.CompilerParams(
            collective_id=0,
            has_side_effects=True,
            vmem_limit_bytes=50 * 1024 * 1024,
        ),
    )(
        grad_terms,
        pltpu.with_memory_space_constraint(row_moment, pltpu.HBM),
        pltpu.with_memory_space_constraint(col_moment, pltpu.HBM),
    )
    return pl.pallas_call(
        finish_kernel,
        out_shape=(shapes[0], shapes[2], shapes[3]),
        in_specs=[vmem] * 4,
        out_specs=(hbm, hbm, hbm),
        scratch_shapes=[pltpu.VMEM((rows, width), f32), dma((8,))],
        compiler_params=pltpu.CompilerParams(vmem_limit_bytes=4 * 1024 * 1024),
    )(scaled, factor, new_rows, new_cols)


def solution(mesh):
    n_row = mesh.shape["row"]
    core = 2 if n_row > 1 else 1
    torus = Mesh(
        mesh.devices.reshape(n_row // core, core, RING, RING), ROW + COL
    )
    in_specs = (P(COL, None, ROW, None), P(None, ROW), P(None, COL))
    out_specs = (P(None, ROW, COL), P(None, ROW), P(None, COL))
    return jax.shard_map(
        on_device, mesh=torus, in_specs=in_specs, out_specs=out_specs, check_vma=False
    )
```
